768 devices in a mesh: shard: 24 (over z, y_lo), replica: 32 (over x, y_hi, core).
Axes of the slice: x: 4, y: 8 (y_hi: 4, y_lo: 2; y = y_hi * 2 + y_lo), z: 12, core: 2. Of those that a mesh axis runs over, the one named last changes fastest.
Arguments:
- atom_feats: bfloat16 [49152, 9, 128], P(('shard', 'replica')), may hold values from -6 to 6
- cotangent: bfloat16 [49152, 9, 128], P(('shard', 'replica')), may hold values from -6 to 6
- frames: bfloat16 [9, 9, 196608], P(None, None, ('shard', 'replica')), may hold values from -2 to 2
- radial: bfloat16 [196608, 128], P(('shard', 'replica')), may hold values from 0.19921875 to 2
- edge_source: int32 [196608], P(('shard', 'replica')), may hold values from 0 to 63
- edge_target: int32 [196608], P(('shard', 'replica')), may hold values from 0 to 63
- edge_valid: int32 [196608], P(('shard', 'replica')), may hold values 0 or 1
- atom_types: int32 [49152], P(('shard', 'replica')), may hold values from 0 to 99
- dataset: int32 [768], P(('shard', 'replica')), may hold values from 0 to 4
- type_table: float32 [100, 128], replicated, may hold values from -6 to 6
- dataset_table: float32 [5, 128], replicated, may hold values from -6 to 6
- router_weight: float32 [128, 28], replicated, may hold values from -1.5 to 1.5
- experts: bfloat16 [28, 384, 384], P(None, 'shard'), may hold values from -3 to 3
Outputs:
- updated: bfloat16 [49152, 9, 128], P(('shard', 'replica'))
- feats_grad: float32 [49152, 9, 128], P(('shard', 'replica'))
- expert_grad: float32 [28, 384, 384], P(None, 'shard')
The draws below stay inside these ranges and needn't reach their ends.
Inputs may be any that keep to these rules, and one draw needn't show every extreme that they name: `edge_source`: indices of atoms within the edge's own system. `edge_target`: indices of atoms within the edge's own system.
All inputs are finite; a program needn't handle non-finite values. No bound on the sum of `edge_valid` on one device may be relied on, other than what follows from the above.
Results may differ from the reference program's by a relative error of at most 0.011.
Values may be sent and summed in bfloat16 or wider, within the bound.
No kernel may reach another device: no remote copies, remote signals or barrier semaphores. Data moves between devices by JAX's collectives and lax.ppermute only.
A program may use at most 64 MiB of HBM per device.

```python
import math
import jax
import jax.numpy as jnp
import numpy as np
from jax import lax

C = 128
LMAX = 2
EXPERTS = 28
TYPES = 100
DATASETS = 5
A_DEV = 64
E_DEV = 256
COEFS = 9
SYSTEMS = 768
ATOMS = 49152
EDGES = 196608
N_SHARD = 24
N_REPLICA = 32


def with_ends(array, own_key, least, top_value):
    index_at = [jax.random.randint(jax.random.fold_in(own_key, axis), (), 0, length) for axis, length in enumerate(array.shape)]
    longest = array.shape.index(max(array.shape))
    beside = index_at[:longest] + [(index_at[longest] + 1) % array.shape[longest]] + index_at[longest + 1:]
    return array.at[tuple(index_at)].set(least).at[tuple(beside)].set(top_value)


def shard_levels(rng, extent, pieces, smallest, largest):
    gain = 1.0
    for dim, shards_of in pieces:
        steps = jax.random.uniform(jax.random.fold_in(jax.random.fold_in(rng, 6), dim), (shards_of,), jnp.float32, smallest / len(pieces), largest / len(pieces))
        gain = gain * jnp.repeat(jnp.exp(steps), extent[dim] // shards_of).reshape((-1,) + (1,) * (len(extent) - 1 - dim))
    return gain


def rank_bounds(amount, skew):
    loads = [(1 << 20) // math.isqrt(grade ** skew) + 1 for grade in range(1, amount + 1)]
    deviation = 1 + sum(loads) // (1 << 30)
    return np.cumsum(np.array([max(1, weight // deviation) for weight in loads]))


def skewed_ids(key, extent, number_of, lean):
    grid = rank_bounds(number_of, lean)
    ticket = jax.random.randint(jax.random.fold_in(key, 1), extent, 0, int(grid[number_of - 1]))
    standing = jnp.searchsorted(jnp.asarray(grid, jnp.int32), ticket, side="right")
    return jax.random.permutation(jax.random.fold_in(key, 2), number_of)[standing].astype(jnp.int32)


def scatter_about(key, extent, deviation, most, shards=(), kind=jnp.bfloat16):
    level = shard_levels(key, extent, shards, -0.22, 0.18) if shards else 1.0
    array = jax.random.normal(key, extent, jnp.float32) * deviation * level
    return jnp.minimum(jnp.maximum(array, -most), most).astype(kind)


def setup_inputs(seed: int = 0) -> dict:
    keys = jax.random.split(jax.random.key(seed), 14)
    return {
        "atom_feats": scatter_about(keys[0], (ATOMS, COEFS, C), 1.0, 6.0, ((0, 768),)),
        "cotangent": scatter_about(keys[1], (ATOMS, COEFS, C), 1.0, 6.0, ((0, 768),)),
        "frames": scatter_about(keys[2], (COEFS, COEFS, EDGES), COEFS ** -0.5, 2.0, ((2, 768),)),
        "radial": jnp.clip(jnp.exp(math.log(2.0) - 2.306499 * jax.random.uniform(keys[3], (EDGES, C), jnp.float32) ** shard_levels(keys[3], (EDGES, C), ((0, 768),), -0.2, 0.2)), 0.19921875, 2.0).astype(jnp.bfloat16),
        "edge_source": with_ends(jax.random.randint(keys[4], (EDGES,), 0, A_DEV), jax.random.fold_in(keys[4], 1), 0, A_DEV - 1).astype(jnp.int32),
        "edge_target": with_ends(jax.random.randint(keys[5], (EDGES,), 0, A_DEV), jax.random.fold_in(keys[5], 1), 0, A_DEV - 1).astype(jnp.int32),
        "edge_valid": with_ends((jax.random.randint(keys[6], (EDGES,), 0, 8) < 7).astype(jnp.int32), jax.random.fold_in(keys[6], 1), 0, 1),
        "atom_types": with_ends(skewed_ids(keys[7], (ATOMS,), TYPES, 2), jax.random.fold_in(keys[7], 3), 0, TYPES - 1).astype(jnp.int32),
        "dataset": with_ends(jax.random.randint(keys[8], (SYSTEMS,), 0, DATASETS), jax.random.fold_in(keys[8], 1), 0, DATASETS - 1).astype(jnp.int32),
        "type_table": scatter_about(keys[9], (TYPES, C), 1.0, 6.0, (), jnp.float32),
        "dataset_table": scatter_about(keys[10], (DATASETS, C), 1.0, 6.0, (), jnp.float32),
        "router_weight": scatter_about(keys[11], (C, EXPERTS), (C // 8) ** -0.5, 1.5, (), jnp.float32),
        "experts": scatter_about(keys[12], (EXPERTS, (LMAX + 1) * C, (LMAX + 1) * C), (4.0 / ((LMAX + 1) * C) ** 0.5), 3.0, ((1, 24),)),
    }


def system_mix(type_rows, dataset_one, type_table, dataset_table, router_weight):
    table_size = type_table.shape[0]
    onehot = (type_rows[:, None] == jnp.arange(table_size, dtype=jnp.int32)[None, :]).astype(jnp.float32)
    counts = lax.optimization_barrier(jnp.sum(onehot, axis=0))
    embed = jnp.dot(counts, type_table, precision=lax.Precision.HIGHEST) / type_rows.shape[0]
    pick = (dataset_one[:, None] == jnp.arange(dataset_table.shape[0], dtype=jnp.int32)[None, :]).astype(jnp.float32)
    embed = embed + jnp.dot(pick, dataset_table, precision=lax.Precision.HIGHEST)[0]
    soft = jax.nn.softplus(jnp.dot(embed, router_weight, precision=lax.Precision.HIGHEST))
    return soft / jnp.sum(soft)

def edge_layer(feats32, merged32, frames, radial, source, target, valid):
    atom_count, components, channels = feats32.shape
    edge_count = source.shape[0]
    top_degree = math.isqrt(components) - 1
    feats = feats32.astype(jnp.bfloat16)
    merged = merged32.astype(jnp.bfloat16)
    gathered = jnp.take(feats, source, axis=0)
    rotated = jnp.einsum('ije,ejc->eic', frames.astype(jnp.float32), gathered.astype(jnp.float32)).astype(jnp.bfloat16)
    zero_rows = [degree * degree + degree for degree in range(top_degree + 1)]
    zero_band = jnp.concatenate([rotated[:, row:row + 1, :] for row in zero_rows], axis=1).reshape(edge_count, -1)
    mixed_band = jnp.dot(zero_band, merged, preferred_element_type=jnp.float32).reshape(edge_count, top_degree + 1, channels)
    columns = []
    for column in range(components):
        if column in zero_rows:
            columns.append(mixed_band[:, zero_rows.index(column), :])
        else:
            columns.append(rotated[:, column, :].astype(jnp.float32))
    combined = jnp.stack(columns, axis=1)
    message = (combined * radial.astype(jnp.float32)[:, None, :]).astype(jnp.bfloat16)
    unrotated = jnp.einsum('jie,ejc->eic', frames.astype(jnp.float32), message.astype(jnp.float32)).astype(jnp.bfloat16)
    incidence = ((target[None, :] == jnp.arange(atom_count, dtype=jnp.int32)[:, None]) & (valid[None, :] > 0)).astype(jnp.bfloat16)
    summed = jnp.dot(incidence, unrotated.reshape(edge_count, -1), preferred_element_type=jnp.float32)
    return feats32 + summed.reshape(atom_count, components, channels) * (atom_count / edge_count)

def reference(atom_feats, cotangent, frames, radial, edge_source, edge_target, edge_valid, atom_types, dataset, type_table, dataset_table, router_weight, experts):
    count = N_SHARD * N_REPLICA
    comps = atom_feats.shape[1]
    feats_sys = atom_feats.reshape(count, A_DEV, comps, C)
    cot_sys = cotangent.reshape(count, A_DEV, comps, C)
    frames_sys = jnp.moveaxis(frames.reshape(comps, comps, count, E_DEV), 2, 0)
    radial_sys = radial.reshape(count, E_DEV, C)
    source_sys = edge_source.reshape(count, E_DEV)
    target_sys = edge_target.reshape(count, E_DEV)
    valid_sys = edge_valid.reshape(count, E_DEV)
    types_sys = atom_types.reshape(count, A_DEV)
    data_sys = dataset.reshape(count, 1)
    experts32 = experts.astype(jnp.float32)

    def one_system(total, inputs):
        feats, cot, frame, rad, source, target, valid, types, data_one = inputs
        mixture = system_mix(types, data_one, type_table, dataset_table, router_weight)
        merged = jnp.einsum('k,krc->rc', mixture, experts32, precision=lax.Precision.HIGHEST).astype(jnp.bfloat16)
        merged32 = lax.optimization_barrier(merged).astype(jnp.float32)

        def local(feats32, weight32):
            return edge_layer(feats32, weight32, frame, rad, source, target, valid)
        result, pullback = jax.vjp(local, feats.astype(jnp.float32), merged32)
        grad_feats, weight_grad = pullback(cot.astype(jnp.float32))
        partial_value = lax.optimization_barrier((mixture[:, None, None] * weight_grad[None]).astype(jnp.bfloat16))
        return (total + partial_value.astype(jnp.float32), (result.astype(jnp.bfloat16), grad_feats))
    start = jnp.zeros(experts.shape, jnp.float32)
    total, (updated, grads) = lax.scan(one_system, start, (feats_sys, cot_sys, frames_sys, radial_sys, source_sys, target_sys, valid_sys, types_sys, data_sys))
    return (updated.reshape(atom_feats.shape), grads.reshape(atom_feats.shape), total)
```

```python
import math

import jax
import jax.numpy as jnp
from jax import lax
from jax.experimental import pallas as pl
from jax.experimental.pallas import tpu as pltpu
from jax.sharding import PartitionSpec as P

BF16 = jnp.bfloat16
F32 = jnp.float32
CHUNK = 16
PARTS = 3


def iota(shape, dim):
    return lax.broadcasted_iota(jnp.int32, shape, dim)


def dot(a, b, contract):
    return lax.dot_general(a, b, ((contract[:1], contract[1:]), ((), ())), preferred_element_type=F32)


def one_hot(index_row, count):
    return iota((count, index_row.shape[1]), 0) == index_row


def split(value):
    parts = []
    for _ in range(PARTS):
        part = value.astype(BF16)
        parts.append(part)
        value = value - part.astype(F32)
    return parts


def mixture_row(types_ref, dataset_ref, type_table_ref, dataset_table_ref, router_ref):
    table = type_table_ref[...]
    atoms = types_ref.shape[1]
    counts = jnp.sum(one_hot(types_ref[...], table.shape[0]).astype(F32), axis=1, keepdims=True)
    embed = jnp.sum(counts * table, axis=0, keepdims=True) / atoms
    data_table = dataset_table_ref[...]
    pick = (iota((data_table.shape[0], 1), 0) == dataset_ref[...]).astype(F32)
    embed = embed + jnp.sum(pick * data_table, axis=0, keepdims=True)
    logits = jnp.sum(router_ref[...] * embed, axis=1, keepdims=True)
    soft = jnp.maximum(logits, 0.0) + jnp.log1p(jnp.exp(-jnp.abs(logits)))
    mixture = soft / jnp.sum(soft, axis=0, keepdims=True)
    shape = (mixture.shape[0], 128)
    return jnp.sum(jnp.where(iota(shape, 0) == iota(shape, 1), mixture, 0.0), axis=0, keepdims=True)


def spread(feats_ref, cot_ref, source_ref, target_ref, valid_ref, gathered_ref, back_ref, scale):
    atoms = feats_ref.shape[1]
    source = one_hot(source_ref[...], atoms).astype(BF16)
    incidence = (one_hot(target_ref[...], atoms) & (valid_ref[...] > 0)).astype(BF16)
    for j in range(feats_ref.shape[0]):
        gathered_ref[j] = dot(feats_ref[j], source, (0, 0))
        back_ref[j] = dot(cot_ref[j], incidence, (0, 0)) * scale
    return source, incidence


def rotate(frames_ref, rows, values, transposed=False):
    count = len(values)
    out = []
    for i in rows:
        total = None
        for j in range(count):
            row = frames_ref[j, i : i + 1, :] if transposed else frames_ref[i, j : j + 1, :]
            term = row * values[j]
            total = term if total is None else total + term
        out.append(total)
    return out


def first_kernel(
    group,
    zero_rows,
    scale,
    feats_ref,
    cot_ref,
    frames_ref,
    radial_ref,
    source_ref,
    target_ref,
    valid_ref,
    types_ref,
    dataset_ref,
    type_table_ref,
    dataset_table_ref,
    router_ref,
    out_ref,
    frames32_ref,
    gathered_ref,
    back_ref,
    gate_ref,
    band_ref,
    mixed_ref,
):
    comps, _, channels = feats_ref.shape
    frames32_ref[...] = frames_ref[...].astype(F32)
    gate_ref[...] = radial_ref[...].astype(F32).T
    spread(feats_ref, cot_ref, source_ref, target_ref, valid_ref, gathered_ref, back_ref, scale)

    def chunk(step, carry):
        at = pl.ds(pl.multiple_of(step * CHUNK, CHUNK), CHUNK)
        values = [gathered_ref[j, at, :] for j in range(comps)]
        for n, total in enumerate(rotate(frames32_ref, zero_rows, values)):
            band_ref[n, at, :] = total.astype(BF16)
        values = [back_ref[j, at, :] for j in range(comps)]
        gate = gate_ref[at, :]
        for n, total in enumerate(rotate(frames32_ref, zero_rows, values)):
            mixed_ref[n, at, :] = (total.astype(BF16).astype(F32) * gate).astype(BF16)
        return carry

    lax.fori_loop(0, channels // CHUNK, chunk, 0)
    width = len(zero_rows) * channels
    edges = band_ref.shape[2]
    band = band_ref[...].reshape(width, edges)
    block = width // group
    for n in range(len(zero_rows)):
        grad = dot(band, mixed_ref[n], (1, 1)).astype(BF16)
        out_ref[:, n * block : (n + 1) * block, :] = grad.reshape(group, block, channels)
    row = mixture_row(types_ref, dataset_ref, type_table_ref, dataset_table_ref, router_ref)
    spare = out_ref.shape[1] - len(zero_rows) * block
    tail = jnp.concatenate(
        [part.astype(F32) for part in split(row)] + [jnp.zeros((spare - PARTS, channels), F32)], axis=0
    ).astype(BF16)
    out_ref[:, len(zero_rows) * block :, :] = jnp.broadcast_to(tail[None], (group, spare, channels))


def second_kernel(experts_count, recv_ref, experts_ref, shares_ref, sums_ref):
    group, lines, channels = recv_ref.shape
    total_rows, width = experts_ref.shape
    block = total_rows // experts_count
    pieces = width // channels
    rows = group * block
    tail = recv_ref[:, pieces * block :, :].astype(F32)
    spread_systems = (iota((rows, group), 0) // block == iota((rows, group), 1)).astype(BF16)
    spread_experts = (iota((channels, total_rows), 1) // block == iota((channels, total_rows), 0)).astype(BF16)
    collect_experts = (iota((total_rows, channels), 0) // block == iota((total_rows, channels), 1)).astype(BF16)
    collect_systems = (iota((group, rows), 1) // block == iota((group, rows), 0)).astype(BF16)
    same = iota((rows, total_rows), 0) % block == iota((rows, total_rows), 1) % block
    same_back = iota((total_rows, rows), 0) % block == iota((total_rows, rows), 1) % block
    experts = experts_ref[...]
    shares = None
    back = []
    for p in range(PARTS):
        part = tail[:, p, :].astype(BF16)
        wide = dot(dot(spread_systems, part, (1, 0)).astype(BF16), spread_experts, (1, 0))
        wide = jnp.where(same, wide, 0.0).astype(BF16)
        term = dot(wide, experts, (1, 0))
        shares = term if shares is None else shares + term
        if p < 2:
            wide = dot(dot(collect_experts, part, (1, 1)).astype(BF16), collect_systems, (1, 0))
            back.append(jnp.where(same_back, wide, 0.0).astype(BF16))
    shares_ref[...] = shares.astype(BF16).reshape(shares_ref.shape)
    for n in range(pieces):
        grads = recv_ref[:, n * block : (n + 1) * block, :].reshape(rows, channels)
        total = dot(back[0], grads, (1, 0)) + dot(back[1], grads, (1, 0))
        sums_ref[:experts_count, :, n * channels : (n + 1) * channels] = total.astype(BF16).reshape(
            experts_count, block, channels
        )
    spare = sums_ref.shape[0] - experts_count
    if spare:
        sums_ref[experts_count:] = jnp.zeros((spare, *sums_ref.shape[1:]), BF16)


def sum_kernel(parts_ref, out_ref):
    total = jnp.sum(parts_ref[...].astype(F32), axis=0)
    out_ref[...] = jnp.broadcast_to(total.astype(BF16)[None], out_ref.shape)


def layer_kernel(
    zero_rows,
    scale,
    feats_ref,
    cot_ref,
    frames_ref,
    radial_ref,
    source_ref,
    target_ref,
    valid_ref,
    merged_ref,
    updated_ref,
    grad_ref,
    frames32_ref,
    gathered_ref,
    back_ref,
    gate_ref,
    rotated_ref,
    turned_ref,
    mixed_ref,
    band_grad_ref,
):
    comps, _, channels = feats_ref.shape
    edges = radial_ref.shape[0]
    width = merged_ref.shape[0]
    frames32_ref[...] = frames_ref[...].astype(F32)
    gate_ref[...] = radial_ref[...].astype(F32).T
    source, incidence = spread(
        feats_ref, cot_ref, source_ref, target_ref, valid_ref, gathered_ref, back_ref, scale
    )

    def forth(step, carry):
        at = pl.ds(pl.multiple_of(step * CHUNK, CHUNK), CHUNK)
        values = [gathered_ref[j, at, :] for j in range(comps)]
        for n, total in enumerate(rotate(frames32_ref, range(comps), values)):
            rotated_ref[n, at, :] = total.astype(BF16)
        values = [back_ref[j, at, :] for j in range(comps)]
        gate = gate_ref[at, :]
        for n, total in enumerate(rotate(frames32_ref, range(comps), values)):
            turned_ref[n, at, :] = (total.astype(BF16).astype(F32) * gate).astype(BF16)
        return carry

    lax.fori_loop(0, channels // CHUNK, forth, 0)
    merged = merged_ref[...]
    band = jnp.concatenate([rotated_ref[row] for row in zero_rows], axis=0)
    mixed_ref[...] = dot(merged, band, (0, 0)).reshape(len(zero_rows), channels, edges)
    turned = jnp.concatenate([turned_ref[row] for row in zero_rows], axis=0)
    band_grad_ref[...] = dot(merged, turned, (1, 0)).astype(BF16).reshape(len(zero_rows), channels, edges)

    def back(step, carry):
        at = pl.ds(pl.multiple_of(step * CHUNK, CHUNK), CHUNK)
        gate = gate_ref[at, :]
        values = []
        for row in range(comps):
            if row in zero_rows:
                value = mixed_ref[zero_rows.index(row), at, :]
            else:
                value = rotated_ref[row, at, :].astype(F32)
            values.append((value * gate).astype(BF16).astype(F32))
        for n, total in enumerate(rotate(frames32_ref, range(comps), values, True)):
            gathered_ref[n, at, :] = total
        values = []
        for row in range(comps):
            if row in zero_rows:
                values.append(band_grad_ref[zero_rows.index(row), at, :].astype(F32))
            else:
                values.append(turned_ref[row, at, :].astype(F32))
        for n, total in enumerate(rotate(frames32_ref, range(comps), values, True)):
            back_ref[n, at, :] = total
        return carry

    lax.fori_loop(0, channels // CHUNK, back, 0)
    for j in range(comps):
        summed = dot(incidence, gathered_ref[j].astype(BF16), (1, 1))
        updated_ref[j] = (feats_ref[j].astype(F32) + summed * scale).astype(BF16)
        summed = dot(source, back_ref[j].astype(BF16), (1, 1))
        grad_ref[j] = cot_ref[j].astype(F32) + summed.astype(BF16).astype(F32)


def call(kernel, outs, scratch, flops, *args):
    size = sum(math.prod(a.shape) * a.dtype.itemsize for a in (*args, *outs))
    return pl.pallas_call(
        kernel,
        out_shape=outs,
        in_specs=[pl.BlockSpec(memory_space=pltpu.VMEM)] * len(args),
        out_specs=[pl.BlockSpec(memory_space=pltpu.VMEM)] * len(outs),
        scratch_shapes=scratch,
        cost_estimate=pl.CostEstimate(flops=flops, bytes_accessed=size, transcendentals=0),
        compiler_params=pltpu.CompilerParams(vmem_limit_bytes=32 * 1024 * 1024),
    )(*args)


def shards(
    atom_feats,
    cotangent,
    frames,
    radial,
    edge_source,
    edge_target,
    edge_valid,
    atom_types,
    dataset,
    type_table,
    dataset_table,
    router_weight,
    experts,
):
    group = lax.axis_size("shard")
    replicas = lax.axis_size("replica")
    expert_count, block, width = experts.shape
    atoms, comps, channels = atom_feats.shape
    edges = radial.shape[0]
    degrees = math.isqrt(comps)
    zero_rows = [degree * degree + degree for degree in range(degrees)]
    scale = atoms / edges
    feats = atom_feats.transpose(1, 0, 2)
    cot = cotangent.transpose(1, 0, 2)
    edge_args = (
        feats,
        cot,
        frames,
        radial,
        edge_source[None],
        edge_target[None],
        edge_valid[None],
    )
    planes = (comps, channels, edges)
    bands = (degrees, channels, edges)
    common = [
        pltpu.VMEM(frames.shape, F32),
        pltpu.VMEM(planes, F32),
        pltpu.VMEM(planes, F32),
        pltpu.VMEM((channels, edges), F32),
    ]

    def first(*refs):
        first_kernel(group, zero_rows, scale, *refs)

    lines = degrees * block + 8
    (sent,) = call(
        first,
        [jax.ShapeDtypeStruct((group, lines, channels), BF16)],
        common + [pltpu.VMEM(bands, BF16), pltpu.VMEM(bands, BF16)],
        10**9,
        *edge_args,
        atom_types[None],
        dataset[None],
        type_table,
        dataset_table,
        router_weight.T,
    )
    received = lax.all_to_all(sent, "shard", 0, 0, tiled=True)

    def second(*refs):
        second_kernel(expert_count, *refs)

    shares, sums = call(
        second,
        [
            jax.ShapeDtypeStruct((group, block, width), BF16),
            jax.ShapeDtypeStruct((replicas, block, width), BF16),
        ],
        [],
        10**9,
        received,
        experts.reshape(expert_count * block, width),
    )
    merged = lax.all_to_all(shares, "shard", 0, 0, tiled=True).reshape(group * block, width)
    parts = lax.all_to_all(sums, "replica", 0, 0, tiled=True)
    (own,) = call(sum_kernel, [jax.ShapeDtypeStruct(parts.shape, BF16)], [], 10**7, parts)
    whole = lax.all_to_all(own, "replica", 0, 0, tiled=True)
    expert_grad = whole[:expert_count].astype(F32)

    def layer(*refs):
        layer_kernel(zero_rows, scale, *refs)

    updated, feats_grad = call(
        layer,
        [jax.ShapeDtypeStruct(feats.shape, BF16), jax.ShapeDtypeStruct(feats.shape, F32)],
        common
        + [
            pltpu.VMEM(planes, BF16),
            pltpu.VMEM(planes, BF16),
            pltpu.VMEM(bands, F32),
            pltpu.VMEM(bands, BF16),
        ],
        5 * 10**9,
        *edge_args,
        merged,
    )
    return (updated.transpose(1, 0, 2), feats_grad.transpose(1, 0, 2), expert_grad)


def solution(mesh):
    both = ("shard", "replica")
    in_specs = (
        P(both, None, None),
        P(both, None, None),
        P(None, None, both),
        P(both, None),
        P(both),
        P(both),
        P(both),
        P(both),
        P(both),
        P(),
        P(),
        P(),
        P(None, "shard", None),
    )
    out_specs = (P(both, None, None), P(both, None, None), P(None, "shard", None))
    return jax.shard_map(shards, mesh=mesh, in_specs=in_specs, out_specs=out_specs, check_vma=False)
```

```python
import math

import jax
import jax.numpy as jnp
from jax import lax
from jax.experimental import pallas as pl
from jax.experimental.pallas import tpu as pltpu
from jax.sharding import Mesh
from jax.sharding import PartitionSpec as P


BF16 = jnp.bfloat16
F32 = jnp.float32
CHUNK = 16
PARTS = 3
REPLICA_SIZES = (4, 4, 2)


def iota(shape, dim):
    return lax.broadcasted_iota(jnp.int32, shape, dim)


def dot(a, b, contract):
    return lax.dot_general(a, b, ((contract[:1], contract[1:]), ((), ())), preferred_element_type=F32)


def one_hot(index_row, count):
    return iota((count, index_row.shape[1]), 0) == index_row


def split(value):
    parts = []
    for _ in range(PARTS):
        part = value.astype(BF16)
        parts.append(part)
        value = value - part.astype(F32)
    return parts


def mixture_row(types_ref, dataset_ref, type_table_ref, dataset_table_ref, router_ref):
    table = type_table_ref[...]
    atoms = types_ref.shape[1]
    counts = jnp.sum(one_hot(types_ref[...], table.shape[0]).astype(F32), axis=1, keepdims=True)
    embed = jnp.sum(counts * table, axis=0, keepdims=True) / atoms
    data_table = dataset_table_ref[...]
    pick = (iota((data_table.shape[0], 1), 0) == dataset_ref[...]).astype(F32)
    embed = embed + jnp.sum(pick * data_table, axis=0, keepdims=True)
    logits = jnp.sum(router_ref[...] * embed, axis=1, keepdims=True)
    soft = jnp.maximum(logits, 0.0) + jnp.log1p(jnp.exp(-jnp.abs(logits)))
    mixture = soft / jnp.sum(soft, axis=0, keepdims=True)
    shape = (mixture.shape[0], 128)
    return jnp.sum(jnp.where(iota(shape, 0) == iota(shape, 1), mixture, 0.0), axis=0, keepdims=True)


def spread(feats_ref, cot_ref, source_ref, target_ref, valid_ref, gathered_ref, back_ref, scale):
    atoms = feats_ref.shape[1]
    source = one_hot(source_ref[...], atoms).astype(BF16)
    incidence = (one_hot(target_ref[...], atoms) & (valid_ref[...] > 0)).astype(BF16)
    for j in range(feats_ref.shape[0]):
        gathered_ref[j] = dot(feats_ref[j], source, (0, 0))
        back_ref[j] = dot(cot_ref[j], incidence, (0, 0)) * scale
    return source, incidence


def rotate(frames_ref, rows, values, transposed=False):
    count = len(values)
    out = []
    for i in rows:
        total = None
        for j in range(count):
            row = frames_ref[j, i : i + 1, :] if transposed else frames_ref[i, j : j + 1, :]
            term = row * values[j]
            total = term if total is None else total + term
        out.append(total)
    return out


def first_kernel(group, zero_rows, scale, *refs):
    count = 12
    sources, (out_ref,), refs = refs[:count], refs[count : count + 1], refs[count + 1 :]
    inputs, refs = refs[:count], refs[count:]
    frames32_ref, gathered_ref, back_ref, gate_ref, band_ref, mixed_ref, sems = refs
    copies = [
        pltpu.make_async_copy(source, target, sems.at[n])
        for n, (source, target) in enumerate(zip(sources, inputs))
    ]
    for copy in copies:
        copy.start()
    router_args, edge_args = inputs[:5], inputs[5:]
    for copy in copies[:5]:
        copy.wait()
    row = mixture_row(*router_args)
    group_lines = out_ref.shape[1]
    source_ref, target_ref, valid_ref, feats_ref, cot_ref, frames_ref, radial_ref = edge_args
    for copy in copies[5:]:
        copy.wait()
    comps, _, channels = feats_ref.shape
    frames32_ref[...] = frames_ref[...].astype(F32)
    gate_ref[...] = radial_ref[...].astype(F32).T
    spread(feats_ref, cot_ref, source_ref, target_ref, valid_ref, gathered_ref, back_ref, scale)

    def chunk(step, carry):
        at = pl.ds(pl.multiple_of(step * CHUNK, CHUNK), CHUNK)
        values = [gathered_ref[j, at, :] for j in range(comps)]
        for n, total in enumerate(rotate(frames32_ref, zero_rows, values)):
            band_ref[n, at, :] = total.astype(BF16)
        values = [back_ref[j, at, :] for j in range(comps)]
        gate = gate_ref[at, :]
        for n, total in enumerate(rotate(frames32_ref, zero_rows, values)):
            mixed_ref[n, at, :] = (total.astype(BF16).astype(F32) * gate).astype(BF16)
        return carry

    lax.fori_loop(0, channels // CHUNK, chunk, 0)
    width = len(zero_rows) * channels
    edges = band_ref.shape[2]
    band = band_ref[...].reshape(width, edges)
    block = width // group
    for n in range(len(zero_rows)):
        grad = dot(band, mixed_ref[n], (1, 1)).astype(BF16)
        out_ref[:, n * block : (n + 1) * block, :] = grad.reshape(group, block, channels)
    spare = group_lines - len(zero_rows) * block
    tail = jnp.concatenate(
        [part.astype(F32) for part in split(row)] + [jnp.zeros((spare - PARTS, channels), F32)], axis=0
    ).astype(BF16)
    out_ref[:, len(zero_rows) * block :, :] = jnp.broadcast_to(tail[None], (group, spare, channels))


def tail_rows(recv_ref, block):
    channels = recv_ref.shape[2]
    lines = recv_ref.shape[1] - recv_ref.shape[1] % block
    return recv_ref[:, lines:, :].astype(F32), lines // block, channels


def sums_kernel(expert_count, block, order, recv_ref, sums_ref):
    tail, pieces, channels = tail_rows(recv_ref, block)
    group = recv_ref.shape[0]
    rows, total_rows = group * block, expert_count * block
    collect_experts = (iota((total_rows, channels), 0) // block == iota((total_rows, channels), 1)).astype(BF16)
    collect_systems = (iota((group, rows), 1) // block == iota((group, rows), 0)).astype(BF16)
    same = iota((total_rows, rows), 0) % block == iota((total_rows, rows), 1) % block
    weights = []
    for p in range(2):
        part = tail[:, p, :].astype(BF16)
        wide = dot(dot(collect_experts, part, (1, 1)).astype(BF16), collect_systems, (1, 0))
        weights.append(jnp.where(same, wide, 0.0).astype(BF16))
    for n in range(pieces):
        grads = recv_ref[:, n * block : (n + 1) * block, :].reshape(rows, channels)
        total = (dot(weights[0], grads, (1, 0)) + dot(weights[1], grads, (1, 0))).astype(BF16)
        piece = sums_ref.shape[1]
        for member, at in enumerate(order):
            rows_here = max(0, min(piece, total_rows - at * piece))
            lanes = slice(n * channels, (n + 1) * channels)
            if rows_here:
                sums_ref[member, :rows_here, lanes] = total[at * piece : at * piece + rows_here]
            if rows_here < piece:
                sums_ref[member, rows_here:, lanes] = jnp.zeros((piece - rows_here, channels), BF16)


def shares_kernel(block, recv_ref, experts_ref, shares_ref):
    tail, _, channels = tail_rows(recv_ref, block)
    group = recv_ref.shape[0]
    total_rows, _ = experts_ref.shape
    rows = group * block
    spread_systems = (iota((rows, group), 0) // block == iota((rows, group), 1)).astype(BF16)
    spread_experts = (iota((channels, total_rows), 1) // block == iota((channels, total_rows), 0)).astype(BF16)
    same = iota((rows, total_rows), 0) % block == iota((rows, total_rows), 1) % block
    experts = experts_ref[...]
    shares = None
    for p in range(PARTS):
        part = tail[:, p, :].astype(BF16)
        wide = dot(dot(spread_systems, part, (1, 0)).astype(BF16), spread_experts, (1, 0))
        term = dot(jnp.where(same, wide, 0.0).astype(BF16), experts, (1, 0))
        shares = term if shares is None else shares + term
    shares_ref[...] = shares.astype(BF16)


def sum_kernel(parts_ref, out_ref):
    out_ref[...] = jnp.sum(parts_ref[...].astype(F32), axis=0).astype(BF16)


def pair_kernel(own_ref, other_ref, out_ref):
    total = (own_ref[...].astype(F32) + other_ref[...].astype(F32)).astype(BF16)
    out_ref[...] = jnp.broadcast_to(total, out_ref.shape)


def layer_kernel(
    zero_rows,
    scale,
    feats_ref,
    cot_ref,
    frames_ref,
    radial_ref,
    source_ref,
    target_ref,
    valid_ref,
    merged_ref,
    updated_ref,
    grad_ref,
    frames32_ref,
    gathered_ref,
    back_ref,
    gate_ref,
    rotated_ref,
    turned_ref,
    mixed_ref,
    band_grad_ref,
):
    comps, _, channels = feats_ref.shape
    edges = radial_ref.shape[0]
    frames32_ref[...] = frames_ref[...].astype(F32)
    gate_ref[...] = radial_ref[...].astype(F32).T
    source, incidence = spread(
        feats_ref, cot_ref, source_ref, target_ref, valid_ref, gathered_ref, back_ref, scale
    )

    def forth(step, carry):
        at = pl.ds(pl.multiple_of(step * CHUNK, CHUNK), CHUNK)
        values = [gathered_ref[j, at, :] for j in range(comps)]
        for n, total in enumerate(rotate(frames32_ref, range(comps), values)):
            rotated_ref[n, at, :] = total.astype(BF16)
        values = [back_ref[j, at, :] for j in range(comps)]
        gate = gate_ref[at, :]
        for n, total in enumerate(rotate(frames32_ref, range(comps), values)):
            turned_ref[n, at, :] = (total.astype(BF16).astype(F32) * gate).astype(BF16)
        return carry

    lax.fori_loop(0, channels // CHUNK, forth, 0)
    merged = merged_ref[...]
    band = jnp.concatenate([rotated_ref[row] for row in zero_rows], axis=0)
    mixed_ref[...] = dot(merged, band, (0, 0)).reshape(len(zero_rows), channels, edges)
    turned = jnp.concatenate([turned_ref[row] for row in zero_rows], axis=0)
    band_grad_ref[...] = dot(merged, turned, (1, 0)).astype(BF16).reshape(len(zero_rows), channels, edges)

    def back(step, carry):
        at = pl.ds(pl.multiple_of(step * CHUNK, CHUNK), CHUNK)
        gate = gate_ref[at, :]
        values = []
        for row in range(comps):
            if row in zero_rows:
                value = mixed_ref[zero_rows.index(row), at, :]
            else:
                value = rotated_ref[row, at, :].astype(F32)
            values.append((value * gate).astype(BF16).astype(F32))
        for n, total in enumerate(rotate(frames32_ref, range(comps), values, True)):
            gathered_ref[n, at, :] = total
        values = []
        for row in range(comps):
            if row in zero_rows:
                values.append(band_grad_ref[zero_rows.index(row), at, :].astype(F32))
            else:
                values.append(turned_ref[row, at, :].astype(F32))
        for n, total in enumerate(rotate(frames32_ref, range(comps), values, True)):
            back_ref[n, at, :] = total
        return carry

    lax.fori_loop(0, channels // CHUNK, back, 0)
    for j in range(comps):
        summed = dot(incidence, gathered_ref[j].astype(BF16), (1, 1))
        updated_ref[j] = (feats_ref[j].astype(F32) + summed * scale).astype(BF16)
        summed = dot(source, back_ref[j].astype(BF16), (1, 1))
        grad_ref[j] = cot_ref[j].astype(F32) + summed.astype(BF16).astype(F32)


def call(kernel, outs, scratch, flops, *args, space=pltpu.VMEM, limit=32 * 1024):
    size = sum(math.prod(a.shape) * a.dtype.itemsize for a in (*args, *outs))
    return pl.pallas_call(
        kernel,
        out_shape=outs,
        in_specs=[pl.BlockSpec(memory_space=space)] * len(args),
        out_specs=[pl.BlockSpec(memory_space=pltpu.VMEM)] * len(outs),
        scratch_shapes=scratch,
        cost_estimate=pl.CostEstimate(flops=flops, bytes_accessed=size, transcendentals=0),
        compiler_params=pltpu.CompilerParams(vmem_limit_bytes=limit * 1024),
    )(*args)


def summed_over_pairs(rows, axis, copies):
    size = lax.axis_size(axis)
    for n, turn in enumerate((1, size - 1)):
        other = lax.ppermute(rows, axis, [(i, i ^ turn) for i in range(size)])
        shape = (copies, *rows.shape) if n else rows.shape
        (rows,) = call(pair_kernel, [jax.ShapeDtypeStruct(shape, BF16)], [], 10**6, rows, other)
    return rows


def shards(
    atom_feats,
    cotangent,
    frames,
    radial,
    edge_source,
    edge_target,
    edge_valid,
    atom_types,
    dataset,
    type_table,
    dataset_table,
    router_weight,
    experts,
):
    group = lax.axis_size("shard")
    expert_count, block, width = experts.shape
    atoms, comps, channels = atom_feats.shape
    edges = radial.shape[0]
    degrees = math.isqrt(comps)
    zero_rows = [degree * degree + degree for degree in range(degrees)]
    scale = atoms / edges
    feats = atom_feats.transpose(1, 0, 2)
    cot = cotangent.transpose(1, 0, 2)
    indices = (edge_source[None], edge_target[None], edge_valid[None])
    planes = (comps, channels, edges)
    bands = (degrees, channels, edges)
    common = [
        pltpu.VMEM(frames.shape, F32),
        pltpu.VMEM(planes, F32),
        pltpu.VMEM(planes, F32),
        pltpu.VMEM((channels, edges), F32),
    ]

    def first(*refs):
        first_kernel(group, zero_rows, scale, *refs)

    lines = degrees * block + 8
    first_args = (
        atom_types[None],
        dataset[None],
        type_table,
        dataset_table,
        router_weight.T,
        *indices,
        feats,
        cot,
        frames,
        radial,
    )
    (sent,) = call(
        first,
        [jax.ShapeDtypeStruct((group, lines, channels), BF16)],
        [pltpu.VMEM(a.shape, a.dtype) for a in first_args]
        + common
        + [pltpu.VMEM(bands, BF16), pltpu.VMEM(bands, BF16), pltpu.SemaphoreType.DMA((len(first_args),))],
        10**9,
        *first_args,
        space=pl.ANY,
        limit=60 * 1024,
    )
    received = lax.all_to_all(sent, "shard", 0, 0, tiled=True)

    def sums_of(*refs):
        sums_kernel(expert_count, block, order, *refs)

    def shares_of(*refs):
        shares_kernel(block, *refs)

    columns, cores = lax.axis_size("x"), lax.axis_size("core")
    line = columns * cores
    piece = -(-expert_count // line) * block
    order = [core * columns + column for column in range(columns) for core in range(cores)]
    (sums,) = call(sums_of, [jax.ShapeDtypeStruct((line, piece, width), BF16)], [], 10**9, received)
    (shares,) = call(
        shares_of,
        [jax.ShapeDtypeStruct((group * block, width), BF16)],
        [],
        10**9,
        received,
        experts.reshape(expert_count * block, width),
    )
    parts = lax.all_to_all(sums, ("x", "core"), 0, 0, tiled=True)
    (own,) = call(sum_kernel, [jax.ShapeDtypeStruct((piece, width), BF16)], [], 10**7, parts)
    merged = lax.all_to_all(shares.reshape(group, block, width), "shard", 0, 0, tiled=True)
    own = summed_over_pairs(own, "y", columns)
    whole = lax.all_to_all(own, "x", 0, 0, tiled=True)

    def layer(*refs):
        layer_kernel(zero_rows, scale, *refs)

    updated, feats_grad = call(
        layer,
        [jax.ShapeDtypeStruct(feats.shape, BF16), jax.ShapeDtypeStruct(feats.shape, F32)],
        common
        + [
            pltpu.VMEM(planes, BF16),
            pltpu.VMEM(planes, BF16),
            pltpu.VMEM(bands, F32),
            pltpu.VMEM(bands, BF16),
        ],
        5 * 10**9,
        feats,
        cot,
        frames,
        radial,
        *indices,
        merged.reshape(group * block, width),
    )
    whole = lax.all_gather(whole.reshape(-1, block, width), "core", axis=0, tiled=True)
    expert_grad = whole[:expert_count].astype(F32)
    return (updated.transpose(1, 0, 2), feats_grad.transpose(1, 0, 2), expert_grad)


def solution(mesh):
    shard_size, replica_size = mesh.devices.shape
    if math.prod(REPLICA_SIZES) != replica_size:
        raise ValueError("replica sizes")
    fine = Mesh(mesh.devices.reshape(shard_size, *REPLICA_SIZES), ("shard", "x", "y", "core"))
    both = ("shard", "x", "y", "core")
    in_specs = (
        P(both, None, None),
        P(both, None, None),
        P(None, None, both),
        P(both, None),
        P(both),
        P(both),
        P(both),
        P(both),
        P(both),
        P(),
        P(),
        P(),
        P(None, "shard", None),
    )
    out_specs = (P(both, None, None), P(both, None, None), P(None, "shard", None))
    return jax.shard_map(shards, mesh=fine, in_specs=in_specs, out_specs=out_specs, check_vma=False)
```

```python
import math

import jax
import jax.numpy as jnp
from jax import lax
from jax.experimental import pallas as pl
from jax.experimental.pallas import tpu as pltpu
from jax.sharding import Mesh
from jax.sharding import PartitionSpec as P


BF16 = jnp.bfloat16
F32 = jnp.float32
CHUNK = 16
PARTS = 3
REPLICA_SIZES = (4, 4, 2)


def iota(shape, dim):
    return lax.broadcasted_iota(jnp.int32, shape, dim)


def dot(a, b, contract):
    return lax.dot_general(a, b, ((contract[:1], contract[1:]), ((), ())), preferred_element_type=F32)


def one_hot(index_row, count):
    return iota((count, index_row.shape[1]), 0) == index_row


def split(value):
    parts = []
    for _ in range(PARTS):
        part = value.astype(BF16)
        parts.append(part)
        value = value - part.astype(F32)
    return parts


def mixture_row(lane, types_ref, dataset_ref, type_table_ref, dataset_table_ref, router_ref):
    table = type_table_ref[...]
    atoms = types_ref.shape[1]
    counts = jnp.sum(one_hot(types_ref[...], table.shape[0]).astype(F32), axis=1, keepdims=True)
    embed = jnp.sum(counts * table, axis=0, keepdims=True) / atoms
    data_table = dataset_table_ref[...]
    pick = (iota((data_table.shape[0], 1), 0) == dataset_ref[...]).astype(F32)
    embed = embed + jnp.sum(pick * data_table, axis=0, keepdims=True)
    logits = jnp.sum(router_ref[...] * embed, axis=1, keepdims=True)
    soft = jnp.maximum(logits, 0.0) + jnp.log1p(jnp.exp(-jnp.abs(logits)))
    mixture = soft / jnp.sum(soft, axis=0, keepdims=True)
    shape = (mixture.shape[0], 128)
    return jnp.sum(jnp.where(iota(shape, 0) + lane == iota(shape, 1), mixture, 0.0), axis=0, keepdims=True)


def spread(feats_ref, cot_ref, source_ref, target_ref, valid_ref, gathered_ref, back_ref, scale):
    atoms = feats_ref.shape[1]
    source = one_hot(source_ref[...], atoms).astype(BF16)
    incidence = (one_hot(target_ref[...], atoms) & (valid_ref[...] > 0)).astype(BF16)
    for j in range(feats_ref.shape[0]):
        gathered_ref[j] = dot(feats_ref[j], source, (0, 0))
        back_ref[j] = dot(cot_ref[j], incidence, (0, 0)) * scale
    return source, incidence


def rotate(frames_ref, rows, values, transposed=False):
    count = len(values)
    out = []
    for i in rows:
        total = None
        for j in range(count):
            row = frames_ref[j, i : i + 1, :] if transposed else frames_ref[i, j : j + 1, :]
            term = row * values[j]
            total = term if total is None else total + term
        out.append(total)
    return out


def first_kernel(zero_rows, scale, *refs):
    count = 12
    sources, (out_ref,), refs = refs[:count], refs[count : count + 1], refs[count + 1 :]
    inputs, refs = refs[:count], refs[count:]
    frames32_ref, gathered_ref, back_ref, gate_ref, band_ref, mixed_ref, sems = refs
    copies = [
        pltpu.make_async_copy(source, target, sems.at[n])
        for n, (source, target) in enumerate(zip(sources, inputs))
    ]
    for copy in copies:
        copy.start()
    router_args, edge_args = inputs[:5], inputs[5:]
    for copy in copies[:5]:
        copy.wait()
    group, columns, block, lanes = out_ref.shape
    slab = band_ref.shape[0] * band_ref.shape[1] // columns
    row = mixture_row(slab, *router_args)
    source_ref, target_ref, valid_ref, feats_ref, cot_ref, frames_ref, radial_ref = edge_args
    for copy in copies[5:]:
        copy.wait()
    comps, _, channels = feats_ref.shape
    frames32_ref[...] = frames_ref[...].astype(F32)
    gate_ref[...] = radial_ref[...].astype(F32).T
    spread(feats_ref, cot_ref, source_ref, target_ref, valid_ref, gathered_ref, back_ref, scale)

    def chunk(step, carry):
        at = pl.ds(pl.multiple_of(step * CHUNK, CHUNK), CHUNK)
        values = [gathered_ref[j, at, :] for j in range(comps)]
        for n, total in enumerate(rotate(frames32_ref, zero_rows, values)):
            band_ref[n, at, :] = total.astype(BF16)
        values = [back_ref[j, at, :] for j in range(comps)]
        gate = gate_ref[at, :]
        for n, total in enumerate(rotate(frames32_ref, zero_rows, values)):
            mixed_ref[n, at, :] = (total.astype(BF16).astype(F32) * gate).astype(BF16)
        return carry

    lax.fori_loop(0, channels // CHUNK, chunk, 0)
    edges = band_ref.shape[2]
    band = band_ref[...].reshape(-1, edges)
    mixed = mixed_ref[...].reshape(-1, edges)
    tail = jnp.concatenate(
        [part.astype(F32) for part in split(row)] + [jnp.zeros((block - PARTS, lanes), F32)], axis=0
    )
    for column in range(columns):
        part = mixed[column * slab : (column + 1) * slab]
        part = jnp.concatenate([part, jnp.zeros((lanes - slab, edges), BF16)], axis=0)
        grad = dot(band, part, (1, 1)).reshape(group, block, lanes) + tail[None]
        out_ref[:, column] = grad.astype(BF16)


def packed_rows(recv_ref, count, start, stride):
    systems, block, lanes = recv_ref.shape
    shape = (count, systems * block)
    pick = (iota(shape, 1) == iota(shape, 0) * stride + start).astype(BF16)
    return dot(pick, recv_ref[...].reshape(systems * block, lanes), (1, 0)).astype(BF16)


def sums_kernel(expert_count, lane, recv_ref, own_ref, send_ref):
    systems, block, lanes = recv_ref.shape
    rows, total_rows = systems * block, expert_count * block
    mixtures = packed_rows(recv_ref, systems, 0, block)
    shape = (total_rows, lanes)
    collect_experts = (iota(shape, 0) // block + lane == iota(shape, 1)).astype(BF16)
    shape = (systems, rows)
    collect_systems = (iota(shape, 1) // block == iota(shape, 0)).astype(BF16)
    wide = dot(dot(collect_experts, mixtures, (1, 1)).astype(BF16), collect_systems, (1, 0))
    same = iota((total_rows, 1), 0) % block == iota((1, rows), 1) % block
    weights = jnp.where(same, wide, 0.0).astype(BF16)
    total = dot(weights, recv_ref[...].reshape(rows, lanes), (1, 0))
    half = own_ref.shape[0]
    first = lax.axis_index("core") == 0
    own_ref[...] = jnp.where(first, total[:half], total[half:]).astype(BF16)
    send_ref[...] = jnp.where(first, total[half:], total[:half]).astype(BF16)


def shares_kernel(group, lane, recv_ref, experts_ref, shares_ref):
    systems, block, lanes = recv_ref.shape
    columns = systems // group
    total_rows = experts_ref.shape[0]
    rows = group * block
    shape = (rows, group)
    spread_systems = (iota(shape, 0) // block == iota(shape, 1)).astype(BF16)
    shape = (lanes, total_rows)
    spread_experts = (iota(shape, 1) // block + lane == iota(shape, 0)).astype(BF16)
    same = iota((rows, 1), 0) % block == iota((1, total_rows), 1) % block
    experts = experts_ref[...]
    start = lax.axis_index("x") * block
    shares = None
    for p in range(PARTS):
        part = packed_rows(recv_ref, group, start + p, columns * block)
        wide = dot(dot(spread_systems, part, (1, 0)).astype(BF16), spread_experts, (1, 0))
        term = dot(jnp.where(same, wide, 0.0).astype(BF16), experts, (1, 0))
        shares = term if shares is None else shares + term
    shares_ref[...] = shares.astype(BF16)


def join_kernel(slab, parts_ref, out_ref):
    pieces, half, lanes = parts_ref.shape
    width = out_ref.shape[1]
    columns = width // slab
    shape = (lanes, width)
    for core in range(pieces // columns):
        total = None
        for column in range(columns):
            place = (iota(shape, 0) < slab) & (iota(shape, 0) + column * slab == iota(shape, 1))
            term = dot(parts_ref[core * columns + column], place.astype(BF16), (1, 0))
            total = term if total is None else total + term
        out_ref[core * half : (core + 1) * half] = total


def pair_kernel(own_ref, other_ref, out_ref):
    total = (own_ref[...].astype(F32) + other_ref[...].astype(F32)).astype(BF16)
    out_ref[...] = jnp.broadcast_to(total, out_ref.shape)


def layer_kernel(
    zero_rows,
    scale,
    feats_ref,
    cot_ref,
    frames_ref,
    radial_ref,
    source_ref,
    target_ref,
    valid_ref,
    merged_ref,
    updated_ref,
    grad_ref,
    frames32_ref,
    gathered_ref,
    back_ref,
    gate_ref,
    rotated_ref,
    turned_ref,
    mixed_ref,
    band_grad_ref,
):
    comps, _, channels = feats_ref.shape
    edges = radial_ref.shape[0]
    frames32_ref[...] = frames_ref[...].astype(F32)
    gate_ref[...] = radial_ref[...].astype(F32).T
    source, incidence = spread(
        feats_ref, cot_ref, source_ref, target_ref, valid_ref, gathered_ref, back_ref, scale
    )

    def forth(step, carry):
        at = pl.ds(pl.multiple_of(step * CHUNK, CHUNK), CHUNK)
        values = [gathered_ref[j, at, :] for j in range(comps)]
        for n, total in enumerate(rotate(frames32_ref, range(comps), values)):
            rotated_ref[n, at, :] = total.astype(BF16)
        values = [back_ref[j, at, :] for j in range(comps)]
        gate = gate_ref[at, :]
        for n, total in enumerate(rotate(frames32_ref, range(comps), values)):
            turned_ref[n, at, :] = (total.astype(BF16).astype(F32) * gate).astype(BF16)
        return carry

    lax.fori_loop(0, channels // CHUNK, forth, 0)
    merged = merged_ref[...]
    band = jnp.concatenate([rotated_ref[row] for row in zero_rows], axis=0)
    mixed_ref[...] = dot(merged, band, (0, 0)).reshape(len(zero_rows), channels, edges)
    turned = jnp.concatenate([turned_ref[row] for row in zero_rows], axis=0)
    band_grad_ref[...] = dot(merged, turned, (1, 0)).astype(BF16).reshape(len(zero_rows), channels, edges)

    def back(step, carry):
        at = pl.ds(pl.multiple_of(step * CHUNK, CHUNK), CHUNK)
        gate = gate_ref[at, :]
        values = []
        for row in range(comps):
            if row in zero_rows:
                value = mixed_ref[zero_rows.index(row), at, :]
            else:
                value = rotated_ref[row, at, :].astype(F32)
            values.append((value * gate).astype(BF16).astype(F32))
        for n, total in enumerate(rotate(frames32_ref, range(comps), values, True)):
            gathered_ref[n, at, :] = total
        values = []
        for row in range(comps):
            if row in zero_rows:
                values.append(band_grad_ref[zero_rows.index(row), at, :].astype(F32))
            else:
                values.append(turned_ref[row, at, :].astype(F32))
        for n, total in enumerate(rotate(frames32_ref, range(comps), values, True)):
            back_ref[n, at, :] = total
        return carry

    lax.fori_loop(0, channels // CHUNK, back, 0)
    for j in range(comps):
        summed = dot(incidence, gathered_ref[j].astype(BF16), (1, 1))
        updated_ref[j] = (feats_ref[j].astype(F32) + summed * scale).astype(BF16)
        summed = dot(source, back_ref[j].astype(BF16), (1, 1))
        grad_ref[j] = cot_ref[j].astype(F32) + summed.astype(BF16).astype(F32)


def call(kernel, outs, scratch, flops, *args, space=pltpu.VMEM, limit=32 * 1024):
    size = sum(math.prod(a.shape) * a.dtype.itemsize for a in (*args, *outs))
    return pl.pallas_call(
        kernel,
        out_shape=outs,
        in_specs=[pl.BlockSpec(memory_space=space)] * len(args),
        out_specs=[pl.BlockSpec(memory_space=pltpu.VMEM)] * len(outs),
        scratch_shapes=scratch,
        cost_estimate=pl.CostEstimate(flops=flops, bytes_accessed=size, transcendentals=0),
        compiler_params=pltpu.CompilerParams(vmem_limit_bytes=limit * 1024),
    )(*args)


def summed_over_pairs(axis, own, send, copies):
    size = lax.axis_size(axis)
    turns = sorted({1, size - 1})
    for turn in turns:
        other = lax.ppermute(send, axis, [(i, i ^ turn) for i in range(size)])
        last = turn == turns[-1] and copies > 1
        shape = (copies, *own.shape) if last else own.shape
        (own,) = call(pair_kernel, [jax.ShapeDtypeStruct(shape, BF16)], [], 10**6, own, other)
        send = own
    return own


def shards(
    atom_feats,
    cotangent,
    frames,
    radial,
    edge_source,
    edge_target,
    edge_valid,
    atom_types,
    dataset,
    type_table,
    dataset_table,
    router_weight,
    experts,
):
    group = lax.axis_size("shard")
    expert_count, block, width = experts.shape
    atoms, comps, channels = atom_feats.shape
    edges = radial.shape[0]
    degrees = math.isqrt(comps)
    zero_rows = [degree * degree + degree for degree in range(degrees)]
    scale = atoms / edges
    feats = atom_feats.transpose(1, 0, 2)
    cot = cotangent.transpose(1, 0, 2)
    indices = (edge_source[None], edge_target[None], edge_valid[None])
    planes = (comps, channels, edges)
    bands = (degrees, channels, edges)
    common = [
        pltpu.VMEM(frames.shape, F32),
        pltpu.VMEM(planes, F32),
        pltpu.VMEM(planes, F32),
        pltpu.VMEM((channels, edges), F32),
    ]

    def first(*refs):
        first_kernel(zero_rows, scale, *refs)

    columns, cores = lax.axis_size("x"), lax.axis_size("core")
    slab = width // columns
    lanes = 128
    if slab + expert_count > lanes or slab % 16 or expert_count % cores or width % columns:
        raise ValueError("sizes")
    first_args = (
        atom_types[None],
        dataset[None],
        type_table,
        dataset_table,
        router_weight.T,
        *indices,
        feats,
        cot,
        frames,
        radial,
    )
    (sent,) = call(
        first,
        [jax.ShapeDtypeStruct((group, columns, block, lanes), BF16)],
        [pltpu.VMEM(a.shape, a.dtype) for a in first_args]
        + common
        + [pltpu.VMEM(bands, BF16), pltpu.VMEM(bands, BF16), pltpu.SemaphoreType.DMA((len(first_args),))],
        10**9,
        *first_args,
        space=pl.ANY,
        limit=60 * 1024,
    )
    sent = sent.reshape(group * columns, block, lanes)
    received = lax.all_to_all(sent, ("shard", "x"), 0, 0, tiled=True)

    def sums_of(*refs):
        sums_kernel(expert_count, slab, *refs)

    def shares_of(*refs):
        shares_kernel(group, slab, *refs)

    half = expert_count // cores * block
    piece = jax.ShapeDtypeStruct((half, lanes), BF16)
    own, send = call(sums_of, [piece, piece], [], 10**9, received)
    (shares,) = call(
        shares_of,
        [jax.ShapeDtypeStruct((group * block, width), BF16)],
        [],
        10**9,
        received,
        experts.reshape(expert_count * block, width),
    )
    merged = lax.all_to_all(shares.reshape(group, block, width), "shard", 0, 0, tiled=True)
    own = summed_over_pairs("core", own, send, 1)
    own = summed_over_pairs("y", own, own, columns)
    whole = lax.all_to_all(own, "x", 0, 0, tiled=True)

    def layer(*refs):
        layer_kernel(zero_rows, scale, *refs)

    updated, feats_grad = call(
        layer,
        [jax.ShapeDtypeStruct(feats.shape, BF16), jax.ShapeDtypeStruct(feats.shape, F32)],
        common
        + [
            pltpu.VMEM(planes, BF16),
            pltpu.VMEM(planes, BF16),
            pltpu.VMEM(bands, F32),
            pltpu.VMEM(bands, BF16),
        ],
        5 * 10**9,
        feats,
        cot,
        frames,
        radial,
        *indices,
        merged.reshape(group * block, width),
    )
    whole = lax.all_gather(whole, "core", axis=0, tiled=True)

    def join(*refs):
        join_kernel(slab, *refs)

    out = jax.ShapeDtypeStruct((expert_count * block, width), F32)
    (expert_grad,) = call(join, [out], [], 10**8, whole)
    expert_grad = expert_grad.reshape(expert_count, block, width)
    return (updated.transpose(1, 0, 2), feats_grad.transpose(1, 0, 2), expert_grad)


def solution(mesh):
    shard_size, replica_size = mesh.devices.shape
    if math.prod(REPLICA_SIZES) != replica_size:
        raise ValueError("replica sizes")
    fine = Mesh(mesh.devices.reshape(shard_size, *REPLICA_SIZES), ("shard", "x", "y", "core"))
    both = ("shard", "x", "y", "core")
    in_specs = (
        P(both, None, None),
        P(both, None, None),
        P(None, None, both),
        P(both, None),
        P(both),
        P(both),
        P(both),
        P(both),
        P(both),
        P(),
        P(),
        P(),
        P(None, "shard", None),
    )
    out_specs = (P(both, None, None), P(both, None, None), P(None, "shard", None))
    return jax.shard_map(shards, mesh=fine, in_specs=in_specs, out_specs=out_specs, check_vma=False)
```

```python
import math

import jax
import jax.numpy as jnp
from jax import lax
from jax.experimental import pallas as pl
from jax.experimental.pallas import tpu as pltpu
from jax.sharding import Mesh
from jax.sharding import PartitionSpec as P


BF16 = jnp.bfloat16
F32 = jnp.float32
CHUNK = 16
PARTS = 2
STRIP = 32
REPLICA_SIZES = (4, 4, 2)


def iota(shape, dim):
    return lax.broadcasted_iota(jnp.int32, shape, dim)


def dot(a, b, contract):
    return lax.dot_general(a, b, ((contract[:1], contract[1:]), ((), ())), preferred_element_type=F32)


def one_hot(index_row, count):
    return iota((count, index_row.shape[1]), 0) == index_row


def split(value):
    parts = []
    for _ in range(PARTS):
        part = value.astype(BF16)
        parts.append(part)
        value = value - part.astype(F32)
    return parts


def mixture_row(lane, types_ref, dataset_ref, type_table_ref, dataset_table_ref, router_ref):
    table = type_table_ref[...]
    atoms = types_ref.shape[1]
    counts = jnp.sum(one_hot(types_ref[...], table.shape[0]).astype(F32), axis=1, keepdims=True)
    embed = jnp.sum(counts * table, axis=0, keepdims=True) / atoms
    data_table = dataset_table_ref[...]
    pick = (iota((data_table.shape[0], 1), 0) == dataset_ref[...]).astype(F32)
    embed = embed + jnp.sum(pick * data_table, axis=0, keepdims=True)
    logits = jnp.sum(router_ref[...] * embed, axis=1, keepdims=True)
    soft = jnp.maximum(logits, 0.0) + jnp.log1p(jnp.exp(-jnp.abs(logits)))
    mixture = soft / jnp.sum(soft, axis=0, keepdims=True)
    shape = (mixture.shape[0], 128)
    return jnp.sum(jnp.where(iota(shape, 0) + lane == iota(shape, 1), mixture, 0.0), axis=0, keepdims=True)


def spread(feats_ref, cot_ref, source_ref, target_ref, valid_ref, gathered_ref, back_ref, scale):
    atoms = feats_ref.shape[1]
    source = one_hot(source_ref[...], atoms).astype(BF16)
    incidence = (one_hot(target_ref[...], atoms) & (valid_ref[...] > 0)).astype(BF16)
    for j in range(feats_ref.shape[0]):
        gathered_ref[j] = dot(feats_ref[j], source, (0, 0))
        back_ref[j] = dot(cot_ref[j], incidence, (0, 0)) * scale
    return source, incidence


def rotate(frames_ref, rows, values, transposed=False):
    count = len(values)
    out = []
    for i in rows:
        total = None
        for j in range(count):
            row = frames_ref[j, i : i + 1, :] if transposed else frames_ref[i, j : j + 1, :]
            term = row * values[j]
            total = term if total is None else total + term
        out.append(total)
    return out


def first_kernel(zero_rows, scale, *refs):
    count = 12
    sources, (out_ref,), refs = refs[:count], refs[count : count + 1], refs[count + 1 :]
    inputs, refs = refs[:count], refs[count:]
    frames32_ref, gathered_ref, back_ref, gate_ref, band_ref, mixed_ref, held_ref, sems = refs
    copies = [
        pltpu.make_async_copy(source, target, sems.at[n])
        for n, (source, target) in enumerate(zip(sources, inputs))
    ]
    for copy in copies:
        copy.start()
    router_args, edge_args = inputs[:5], inputs[5:]
    for copy in copies:
        copy.wait()
    group, columns, block, lanes = out_ref.shape
    slab = band_ref.shape[0] * band_ref.shape[1] // columns
    row = mixture_row(slab, *router_args)
    source_ref, target_ref, valid_ref, feats_ref, cot_ref, frames_ref, radial_ref = edge_args
    comps, _, channels = feats_ref.shape
    frames32_ref[...] = frames_ref[...].astype(F32)
    gate_ref[...] = radial_ref[...].astype(F32).T
    spread(feats_ref, cot_ref, source_ref, target_ref, valid_ref, gathered_ref, back_ref, scale)

    def chunk(step, carry):
        at = pl.ds(pl.multiple_of(step * CHUNK, CHUNK), CHUNK)
        values = [gathered_ref[j, at, :] for j in range(comps)]
        for n, total in enumerate(rotate(frames32_ref, zero_rows, values)):
            band_ref[n, at, :] = total.astype(BF16)
        values = [back_ref[j, at, :] for j in range(comps)]
        gate = gate_ref[at, :]
        for n, total in enumerate(rotate(frames32_ref, zero_rows, values)):
            mixed_ref[n, at, :] = (total.astype(BF16).astype(F32) * gate).astype(BF16)
        return carry

    lax.fori_loop(0, channels // CHUNK, chunk, 0)
    edges = band_ref.shape[2]
    band = band_ref[...].reshape(-1, edges)
    mixed = mixed_ref[...].reshape(-1, edges)
    tail = jnp.concatenate(
        [part.astype(F32) for part in split(row)] + [jnp.zeros((block - PARTS, lanes), F32)], axis=0
    )
    for column in range(columns):
        part = mixed[column * slab : (column + 1) * slab]
        part = jnp.concatenate([part, jnp.zeros((lanes - slab, edges), BF16)], axis=0)
        grad = dot(band, part, (1, 1)).reshape(group, block, lanes) + tail[None]
        held_ref[column] = grad.astype(BF16)
        copies.append(pltpu.make_async_copy(held_ref.at[column], out_ref.at[:, column], sems.at[len(copies)]))
        copies[-1].start()
    for copy in copies[count:]:
        copy.wait()


def packed_rows(recv_ref, count, start, stride):
    systems, block, lanes = recv_ref.shape
    shape = (count, systems * block)
    pick = (iota(shape, 1) == iota(shape, 0) * stride + start).astype(BF16)
    return dot(pick, recv_ref[...].reshape(systems * block, lanes), (1, 0)).astype(BF16)


def sums_kernel(expert_count, lane, recv_ref, own_ref, send_ref):
    systems, block, lanes = recv_ref.shape
    rows, total_rows = systems * block, expert_count * block
    mixtures = packed_rows(recv_ref, systems, 0, block)
    shape = (total_rows, lanes)
    collect_experts = (iota(shape, 0) // block + lane == iota(shape, 1)).astype(BF16)
    shape = (systems, rows)
    collect_systems = (iota(shape, 1) // block == iota(shape, 0)).astype(BF16)
    wide = dot(dot(collect_experts, mixtures, (1, 1)).astype(BF16), collect_systems, (1, 0))
    same = iota((total_rows, 1), 0) % block == iota((1, rows), 1) % block
    weights = jnp.where(same, wide, 0.0).astype(BF16)
    total = dot(weights, recv_ref[...].reshape(rows, lanes), (1, 0))
    half = total_rows // 2
    first = lax.axis_index("core") == 0
    own_ref[...] = packed(jnp.where(first, total[:half], total[half:]), lane)
    send_ref[...] = packed(jnp.where(first, total[half:], total[:half]), lane)


def rolled(value, source, target):
    shift = (target - source) * STRIP % value.shape[1]
    return pltpu.roll(value, shift, 1) if shift else value


def in_strips(strips):
    lane = iota((1, strips[0].shape[1]), 1) // STRIP
    out = strips[0]
    for n, strip in enumerate(strips[1:], 1):
        out = jnp.where(lane == n, strip, out)
    return out


def packed(value, used):
    per = value.shape[1] // STRIP
    rows = value.shape[0] // per
    groups = [value[g * rows : (g + 1) * rows] for g in range(per)]
    blocks = [in_strips([rolled(v, b, g) for g, v in enumerate(groups)]) for b in range(used // STRIP)]
    return jnp.concatenate(blocks, axis=0).astype(BF16)


def shares_kernel(lane, recv_ref, experts_ref, shares_ref, held_ref, sems):
    group, _, block, lanes = recv_ref.shape
    total_rows = experts_ref.shape[0]
    chunks = sems.shape[0]
    rows = group * block // chunks
    tail = recv_ref[:, lax.axis_index("x"), :8, :].astype(F32)
    parts = [tail[:, p, :].astype(BF16) for p in range(PARTS)]
    shape = (lanes, total_rows)
    spread_experts = (iota(shape, 1) // block + lane == iota(shape, 0)).astype(BF16)
    same = iota((rows, 1), 0) % block == iota((1, total_rows), 1) % block
    experts = experts_ref[...]
    wide = [dot(part, spread_experts, (1, 0)).astype(BF16) for part in parts]
    copies = []
    for n in range(chunks):
        at = pl.ds(n * rows, rows)
        shape = (rows, group)
        spread_systems = ((iota(shape, 0) + n * rows) // block == iota(shape, 1)).astype(BF16)
        shares = None
        for part in wide:
            mine = jnp.where(same, dot(spread_systems, part, (1, 0)), 0.0).astype(BF16)
            term = dot(mine, experts, (1, 0))
            shares = term if shares is None else shares + term
        held_ref[at, :] = shares.astype(BF16)
        copies.append(pltpu.make_async_copy(held_ref.at[at, :], shares_ref.at[at, :], sems.at[n]))
        copies[-1].start()
    for copy in copies:
        copy.wait()


def join_kernel(slab, parts_ref, out_ref, held_ref, sems):
    pieces, _, lanes = parts_ref.shape
    half, width = held_ref.shape[1:]
    columns = width // slab
    per = lanes // STRIP
    used = slab // STRIP
    rows = half // per
    copies = []
    for core in range(pieces // columns):
        strips = [
            parts_ref[core * columns + column, b * rows : (b + 1) * rows, :].astype(F32)
            for column in range(columns)
            for b in range(used)
        ]
        for g in range(per):
            for block in range(width // lanes):
                chosen = [rolled(strips[block * per + q], g, q) for q in range(per)]
                held_ref[core, g * rows : (g + 1) * rows, block * lanes : (block + 1) * lanes] = in_strips(chosen)
        copies.append(
            pltpu.make_async_copy(held_ref.at[core], out_ref.at[pl.ds(core * half, half), :], sems.at[core])
        )
        copies[-1].start()
    for copy in copies:
        copy.wait()


def pair_kernel(own_ref, other_ref, out_ref):
    total = (own_ref[...].astype(F32) + other_ref[...].astype(F32)).astype(BF16)
    out_ref[...] = jnp.broadcast_to(total, out_ref.shape)


def layer_kernel(
    zero_rows,
    scale,
    feats_ref,
    cot_ref,
    frames_ref,
    radial_ref,
    source_ref,
    target_ref,
    valid_ref,
    merged_ref,
    updated_ref,
    grad_ref,
    frames32_ref,
    gathered_ref,
    back_ref,
    gate_ref,
    rotated_ref,
    turned_ref,
    mixed_ref,
    band_grad_ref,
):
    comps, _, channels = feats_ref.shape
    edges = radial_ref.shape[0]
    frames32_ref[...] = frames_ref[...].astype(F32)
    gate_ref[...] = radial_ref[...].astype(F32).T
    source, incidence = spread(
        feats_ref, cot_ref, source_ref, target_ref, valid_ref, gathered_ref, back_ref, scale
    )

    def forth(step, carry):
        at = pl.ds(pl.multiple_of(step * CHUNK, CHUNK), CHUNK)
        values = [gathered_ref[j, at, :] for j in range(comps)]
        for n, total in enumerate(rotate(frames32_ref, range(comps), values)):
            rotated_ref[n, at, :] = total.astype(BF16)
        values = [back_ref[j, at, :] for j in range(comps)]
        gate = gate_ref[at, :]
        for n, total in enumerate(rotate(frames32_ref, range(comps), values)):
            turned_ref[n, at, :] = (total.astype(BF16).astype(F32) * gate).astype(BF16)
        return carry

    lax.fori_loop(0, channels // CHUNK, forth, 0)
    merged = merged_ref[...]
    band = jnp.concatenate([rotated_ref[row] for row in zero_rows], axis=0)
    mixed_ref[...] = dot(merged, band, (0, 0)).reshape(len(zero_rows), channels, edges)
    turned = jnp.concatenate([turned_ref[row] for row in zero_rows], axis=0)
    band_grad_ref[...] = dot(merged, turned, (1, 0)).astype(BF16).reshape(len(zero_rows), channels, edges)

    def back(step, carry):
        at = pl.ds(pl.multiple_of(step * CHUNK, CHUNK), CHUNK)
        gate = gate_ref[at, :]
        values = []
        for row in range(comps):
            if row in zero_rows:
                value = mixed_ref[zero_rows.index(row), at, :]
            else:
                value = rotated_ref[row, at, :].astype(F32)
            values.append((value * gate).astype(BF16).astype(F32))
        for n, total in enumerate(rotate(frames32_ref, range(comps), values, True)):
            gathered_ref[n, at, :] = total
        values = []
        for row in range(comps):
            if row in zero_rows:
                values.append(band_grad_ref[zero_rows.index(row), at, :].astype(F32))
            else:
                values.append(turned_ref[row, at, :].astype(F32))
        for n, total in enumerate(rotate(frames32_ref, range(comps), values, True)):
            back_ref[n, at, :] = total
        return carry

    lax.fori_loop(0, channels // CHUNK, back, 0)
    for j in range(comps):
        summed = dot(incidence, gathered_ref[j].astype(BF16), (1, 1))
        updated_ref[j] = (feats_ref[j].astype(F32) + summed * scale).astype(BF16)
        summed = dot(source, back_ref[j].astype(BF16), (1, 1))
        grad_ref[j] = cot_ref[j].astype(F32) + summed.astype(BF16).astype(F32)


def call(kernel, outs, scratch, flops, *args, space=pltpu.VMEM, out_space=pltpu.VMEM, limit=32 * 1024):
    size = sum(math.prod(a.shape) * a.dtype.itemsize for a in (*args, *outs))
    return pl.pallas_call(
        kernel,
        out_shape=outs,
        in_specs=[pl.BlockSpec(memory_space=space)] * len(args),
        out_specs=[pl.BlockSpec(memory_space=out_space)] * len(outs),
        scratch_shapes=scratch,
        cost_estimate=pl.CostEstimate(flops=flops, bytes_accessed=size, transcendentals=0),
        compiler_params=pltpu.CompilerParams(vmem_limit_bytes=limit * 1024),
    )(*args)


def summed_over_pairs(axis, own, send, copies):
    size = lax.axis_size(axis)
    turns = sorted({1, size - 1})
    for turn in turns:
        other = lax.ppermute(send, axis, [(i, i ^ turn) for i in range(size)])
        last = turn == turns[-1] and copies > 1
        shape = (copies, *own.shape) if last else own.shape
        (own,) = call(pair_kernel, [jax.ShapeDtypeStruct(shape, BF16)], [], 10**6, own, other)
        send = own
    return own


def shards(
    atom_feats,
    cotangent,
    frames,
    radial,
    edge_source,
    edge_target,
    edge_valid,
    atom_types,
    dataset,
    type_table,
    dataset_table,
    router_weight,
    experts,
):
    group = lax.axis_size("shard")
    expert_count, block, width = experts.shape
    atoms, comps, channels = atom_feats.shape
    edges = radial.shape[0]
    degrees = math.isqrt(comps)
    zero_rows = [degree * degree + degree for degree in range(degrees)]
    scale = atoms / edges
    feats = atom_feats.transpose(1, 0, 2)
    cot = cotangent.transpose(1, 0, 2)
    indices = (edge_source[None], edge_target[None], edge_valid[None])
    planes = (comps, channels, edges)
    bands = (degrees, channels, edges)
    common = [
        pltpu.VMEM(frames.shape, F32),
        pltpu.VMEM(planes, F32),
        pltpu.VMEM(planes, F32),
        pltpu.VMEM((channels, edges), F32),
    ]

    def first(*refs):
        first_kernel(zero_rows, scale, *refs)

    columns, cores = lax.axis_size("x"), lax.axis_size("core")
    slab = width // columns
    lanes = 128
    half = expert_count // cores * block
    if slab + expert_count > lanes or slab % STRIP or cores != 2 or expert_count % cores or half % (8 * lanes // STRIP):
        raise ValueError("sizes")
    first_args = (
        atom_types[None],
        dataset[None],
        type_table,
        dataset_table,
        router_weight.T,
        *indices,
        feats,
        cot,
        frames,
        radial,
    )
    (sent,) = call(
        first,
        [jax.ShapeDtypeStruct((group, columns, block, lanes), BF16)],
        [pltpu.VMEM(a.shape, a.dtype) for a in first_args]
        + common
        + [
            pltpu.VMEM(bands, BF16),
            pltpu.VMEM(bands, BF16),
            pltpu.VMEM((columns, group, block, lanes), BF16),
            pltpu.SemaphoreType.DMA((len(first_args) + columns,)),
        ],
        10**9,
        *first_args,
        space=pl.ANY,
        out_space=pl.ANY,
        limit=60 * 1024,
    )
    sent = sent.reshape(group * columns, block, lanes)
    received = lax.all_to_all(sent, ("shard", "x"), 0, 0, tiled=True)

    def sums_of(*refs):
        sums_kernel(expert_count, slab, *refs)

    def shares_of(*refs):
        shares_kernel(slab, *refs)

    piece = jax.ShapeDtypeStruct((half * slab // lanes, lanes), BF16)
    own, send = call(sums_of, [piece, piece], [], 10**9, received)
    (shares,) = call(
        shares_of,
        [jax.ShapeDtypeStruct((group * block, width), BF16)],
        [pltpu.VMEM((group * block, width), BF16), pltpu.SemaphoreType.DMA((3,))],
        10**9,
        received.reshape(group, columns, block, lanes),
        experts.reshape(expert_count * block, width),
        out_space=pl.ANY,
    )
    merged = lax.all_to_all(shares.reshape(group, block, width), "shard", 0, 0, tiled=True)
    own = summed_over_pairs("core", own, send, 1)
    own = summed_over_pairs("y", own, own, columns)
    whole = lax.all_to_all(own, "x", 0, 0, tiled=True)

    def layer(*refs):
        layer_kernel(zero_rows, scale, *refs)

    updated, feats_grad = call(
        layer,
        [jax.ShapeDtypeStruct(feats.shape, BF16), jax.ShapeDtypeStruct(feats.shape, F32)],
        common
        + [
            pltpu.VMEM(planes, BF16),
            pltpu.VMEM(planes, BF16),
            pltpu.VMEM(bands, F32),
            pltpu.VMEM(bands, BF16),
        ],
        5 * 10**9,
        feats,
        cot,
        frames,
        radial,
        *indices,
        merged.reshape(group * block, width),
    )
    whole = lax.all_gather(whole, "core", axis=0, tiled=True)

    def join(*refs):
        join_kernel(slab, *refs)

    out = jax.ShapeDtypeStruct((expert_count * block, width), F32)
    scratch = [pltpu.VMEM((cores, half, width), F32), pltpu.SemaphoreType.DMA((cores,))]
    (expert_grad,) = call(join, [out], scratch, 10**8, whole, out_space=pl.ANY)
    expert_grad = expert_grad.reshape(expert_count, block, width)
    return (updated.transpose(1, 0, 2), feats_grad.transpose(1, 0, 2), expert_grad)


def solution(mesh):
    shard_size, replica_size = mesh.devices.shape
    if math.prod(REPLICA_SIZES) != replica_size:
        raise ValueError("replica sizes")
    fine = Mesh(mesh.devices.reshape(shard_size, *REPLICA_SIZES), ("shard", "x", "y", "core"))
    both = ("shard", "x", "y", "core")
    in_specs = (
        P(both, None, None),
        P(both, None, None),
        P(None, None, both),
        P(both, None),
        P(both),
        P(both),
        P(both),
        P(both),
        P(both),
        P(),
        P(),
        P(),
        P(None, "shard", None),
    )
    out_specs = (P(both, None, None), P(both, None, None), P(None, "shard", None))
    return jax.shard_map(shards, mesh=fine, in_specs=in_specs, out_specs=out_specs, check_vma=False)
```

```python
import math

import jax
import jax.numpy as jnp
from jax import lax
from jax.experimental import pallas as pl
from jax.experimental.pallas import tpu as pltpu
from jax.sharding import Mesh
from jax.sharding import PartitionSpec as P


BF16 = jnp.bfloat16
F32 = jnp.float32
CHUNK = 16
PARTS = 2
SUB = 4
REPLICA_SIZES = (4, 4, 2)


def iota(shape, dim):
    return lax.broadcasted_iota(jnp.int32, shape, dim)


def dot(a, b, contract):
    return lax.dot_general(a, b, ((contract[:1], contract[1:]), ((), ())), preferred_element_type=F32)


def divided(value, by):
    return jnp.floor((value.astype(F32) + 0.5) * (1.0 / by)).astype(jnp.int32)


def one_hot(index_row, count):
    return iota((count, index_row.shape[1]), 0) == index_row


def split(value):
    parts = []
    for _ in range(PARTS):
        part = value.astype(BF16)
        parts.append(part)
        value = value - part.astype(F32)
    return parts


def mixture_row(types_ref, dataset_ref, type_table_ref, dataset_table_ref, router_ref):
    table = type_table_ref[...]
    atoms = types_ref.shape[1]
    counts = jnp.sum(one_hot(types_ref[...], table.shape[0]).astype(F32), axis=1, keepdims=True)
    embed = jnp.sum(counts * table, axis=0, keepdims=True) / atoms
    data_table = dataset_table_ref[...]
    pick = (iota((data_table.shape[0], 1), 0) == dataset_ref[...]).astype(F32)
    embed = embed + jnp.sum(pick * data_table, axis=0, keepdims=True)
    logits = jnp.sum(router_ref[...] * embed, axis=1, keepdims=True)
    soft = jnp.maximum(logits, 0.0) + jnp.log1p(jnp.exp(-jnp.abs(logits)))
    mixture = soft / jnp.sum(soft, axis=0, keepdims=True)
    shape = (mixture.shape[0], 128)
    return jnp.sum(jnp.where(iota(shape, 0) == iota(shape, 1), mixture, 0.0), axis=0, keepdims=True)


def spread(feats_ref, cot_ref, source_ref, target_ref, valid_ref, gathered_ref, back_ref, scale):
    atoms = feats_ref.shape[1]
    source = one_hot(source_ref[...], atoms).astype(BF16)
    incidence = (one_hot(target_ref[...], atoms) & (valid_ref[...] > 0)).astype(BF16)
    for j in range(feats_ref.shape[0]):
        gathered_ref[j] = dot(feats_ref[j], source, (0, 0))
        back_ref[j] = dot(cot_ref[j], incidence, (0, 0)) * scale
    return source, incidence


def rotate(frames_ref, rows, values, transposed=False):
    count = len(values)
    out = []
    for i in rows:
        total = None
        for j in range(count):
            row = frames_ref[j, i : i + 1, :] if transposed else frames_ref[i, j : j + 1, :]
            term = row * values[j]
            total = term if total is None else total + term
        out.append(total)
    return out


def first_kernel(zero_rows, scale, *refs):
    count = 12
    sources, (out_ref,), refs = refs[:count], refs[count : count + 1], refs[count + 1 :]
    inputs, refs = refs[:count], refs[count:]
    frames32_ref, gathered_ref, back_ref, gate_ref, band_ref, mixed_ref, held_ref, sems = refs
    copies = [
        pltpu.make_async_copy(source, target, sems.at[n])
        for n, (source, target) in enumerate(zip(sources, inputs))
    ]
    for copy in copies:
        copy.start()
    router_args, edge_args = inputs[:5], inputs[5:]
    for copy in copies:
        copy.wait()
    row = mixture_row(*router_args)
    source_ref, target_ref, valid_ref, feats_ref, cot_ref, frames_ref, radial_ref = edge_args
    comps, _, channels = feats_ref.shape
    frames32_ref[...] = frames_ref[...].astype(F32)
    gate_ref[...] = radial_ref[...].astype(F32).T
    spread(feats_ref, cot_ref, source_ref, target_ref, valid_ref, gathered_ref, back_ref, scale)

    def chunk(step, carry):
        at = pl.ds(pl.multiple_of(step * CHUNK, CHUNK), CHUNK)
        values = [gathered_ref[j, at, :] for j in range(comps)]
        for n, total in enumerate(rotate(frames32_ref, zero_rows, values)):
            band_ref[n, at, :] = total.astype(BF16)
        values = [back_ref[j, at, :] for j in range(comps)]
        gate = gate_ref[at, :]
        for n, total in enumerate(rotate(frames32_ref, zero_rows, values)):
            mixed_ref[n, at, :] = (total.astype(BF16).astype(F32) * gate).astype(BF16)
        return carry

    lax.fori_loop(0, channels // CHUNK, chunk, 0)
    edges = band_ref.shape[2]
    band = band_ref[...].reshape(-1, edges)
    pieces = len(zero_rows)
    grads = [dot(band, mixed_ref[n], (1, 1)).astype(BF16) for n in range(pieces)]
    tail = jnp.concatenate([part.astype(F32) for part in split(row)] + [jnp.zeros((16 - PARTS, channels), F32)], axis=0)
    tail = tail.astype(BF16)
    lines = SUB * pieces + PARTS
    batch = 8
    rows = batch * lines
    line = iota((rows, 1), 0)
    message = divided(line, lines)
    line = line - message * lines
    data = SUB * pieces
    wanted = jnp.where(
        line < data,
        batch * SUB * (line // SUB) + SUB * message + line % SUB,
        batch * data + line - data,
    )
    place = (iota((rows, batch * data + 16), 1) == wanted).astype(BF16)
    steps = band.shape[0] // (batch * SUB)
    chunk_steps = steps // (sems.shape[0] - count)
    for step in range(steps):
        at = slice(step * batch * SUB, (step + 1) * batch * SUB)
        stack = jnp.concatenate([grad[at] for grad in grads] + [tail], axis=0)
        held_ref[step * rows : (step + 1) * rows] = dot(place, stack, (1, 0)).astype(BF16)
        if (step + 1) % chunk_steps == 0:
            done = pl.ds((step + 1 - chunk_steps) * rows, chunk_steps * rows)
            copies.append(pltpu.make_async_copy(held_ref.at[done], out_ref.at[done], sems.at[len(copies)]))
            copies[-1].start()
    for copy in copies[count:]:
        copy.wait()


def sums_kernel(expert_count, group, lines, recv_ref, own_ref, send_ref, mine_ref):
    total_lines, lanes = recv_ref.shape
    systems = total_lines // lines
    columns = systems // group
    data = lines - PARTS
    rows = expert_count * data
    values = recv_ref[...]
    shape = (systems, total_lines)
    picks = [iota(shape, 1) == iota(shape, 0) * lines + data]
    shape = (group, total_lines)
    for p in range(PARTS):
        start = lax.axis_index("x") * lines + data + p
        picks.append(iota(shape, 1) == iota(shape, 0) * (columns * lines) + start)
    picked = dot(jnp.concatenate([pick.astype(F32) for pick in picks], axis=0).astype(BF16), values, (1, 0))
    mine_ref[...] = picked[systems:]
    column = iota((1, total_lines), 1)
    system = divided(column, lines)
    row = iota((rows, 1), 0)
    expert = divided(row, data)
    collect_experts = (iota((rows, lanes), 1) == expert).astype(BF16)
    collect_systems = (iota((systems, total_lines), 0) == system).astype(BF16)
    narrow = dot(collect_experts, picked[:systems].astype(BF16), (1, 1)).astype(BF16)
    same = row - expert * data == column - system * lines
    weights = jnp.where(same, dot(narrow, collect_systems, (1, 0)), 0.0).astype(BF16)
    total = dot(weights, values, (1, 0))
    half = rows // 2
    first = lax.axis_index("core") == 0
    own_ref[...] = jnp.where(first, total[:half], total[half:]).astype(BF16)
    send_ref[...] = jnp.where(first, total[half:], total[:half]).astype(BF16)


def shares_kernel(block, mine_ref, experts_ref, shares_ref, held_ref, sems):
    group = mine_ref.shape[0] // PARTS
    lanes = mine_ref.shape[1]
    total_rows = experts_ref.shape[0]
    chunks = sems.shape[0]
    rows = group * block // chunks
    shape = (lanes, total_rows)
    spread_experts = (iota(shape, 1) // block == iota(shape, 0)).astype(BF16)
    same = iota((rows, 1), 0) % block == iota((1, total_rows), 1) % block
    experts = experts_ref[...]
    parts = [mine_ref[p * group : (p + 1) * group, :].astype(BF16) for p in range(PARTS)]
    wide = [dot(part, spread_experts, (1, 0)).astype(BF16) for part in parts]
    copies = []
    for n in range(chunks):
        at = pl.ds(n * rows, rows)
        shape = (rows, group)
        spread_systems = ((iota(shape, 0) + n * rows) // block == iota(shape, 1)).astype(BF16)
        shares = None
        for part in wide:
            weights = jnp.where(same, dot(spread_systems, part, (1, 0)), 0.0).astype(BF16)
            term = dot(weights, experts, (1, 0))
            shares = term if shares is None else shares + term
        held_ref[at, :] = shares.astype(BF16)
        copies.append(pltpu.make_async_copy(held_ref.at[at, :], shares_ref.at[at, :], sems.at[n]))
        copies[-1].start()
    for copy in copies:
        copy.wait()


def join_kernel(block, parts_ref, out_ref, held_ref, sems):
    cores, half, width = held_ref.shape
    columns = block // SUB
    lanes = parts_ref.shape[2]
    pieces = width // lanes
    data = SUB * pieces
    low = iota((2 * SUB, lanes), 0) < SUB
    copies = []

    def turned(value, line, place):
        at = line // (2 * SUB) * 2 * SUB
        value = value[at : at + 2 * SUB]
        return value if line - at == place else pltpu.roll(value, SUB, 0)

    for core in range(cores):
        values = [parts_ref[core * columns + column].astype(F32) for column in range(columns)]
        for expert in range(half // block):
            for piece in range(pieces):
                line = expert * data + piece * SUB
                for column in range(0, columns, 2):
                    upper = turned(values[column], line, 0)
                    lower = turned(values[column + 1], line, SUB)
                    at = expert * block + column * SUB
                    held_ref[core, at : at + 2 * SUB, piece * lanes : (piece + 1) * lanes] = jnp.where(low, upper, lower)
        copies.append(
            pltpu.make_async_copy(held_ref.at[core], out_ref.at[pl.ds(core * half, half), :], sems.at[core])
        )
        copies[-1].start()
    for copy in copies:
        copy.wait()


def pair_kernel(own_ref, other_ref, out_ref):
    total = (own_ref[...].astype(F32) + other_ref[...].astype(F32)).astype(BF16)
    out_ref[...] = jnp.broadcast_to(total, out_ref.shape)


def layer_kernel(
    zero_rows,
    scale,
    feats_ref,
    cot_ref,
    frames_ref,
    radial_ref,
    source_ref,
    target_ref,
    valid_ref,
    merged_ref,
    updated_ref,
    grad_ref,
    frames32_ref,
    gathered_ref,
    back_ref,
    gate_ref,
    rotated_ref,
    turned_ref,
    mixed_ref,
    band_grad_ref,
):
    comps, _, channels = feats_ref.shape
    edges = radial_ref.shape[0]
    frames32_ref[...] = frames_ref[...].astype(F32)
    gate_ref[...] = radial_ref[...].astype(F32).T
    source, incidence = spread(
        feats_ref, cot_ref, source_ref, target_ref, valid_ref, gathered_ref, back_ref, scale
    )

    def forth(step, carry):
        at = pl.ds(pl.multiple_of(step * CHUNK, CHUNK), CHUNK)
        values = [gathered_ref[j, at, :] for j in range(comps)]
        for n, total in enumerate(rotate(frames32_ref, range(comps), values)):
            rotated_ref[n, at, :] = total.astype(BF16)
        values = [back_ref[j, at, :] for j in range(comps)]
        gate = gate_ref[at, :]
        for n, total in enumerate(rotate(frames32_ref, range(comps), values)):
            turned_ref[n, at, :] = (total.astype(BF16).astype(F32) * gate).astype(BF16)
        return carry

    lax.fori_loop(0, channels // CHUNK, forth, 0)
    merged = merged_ref[...]
    band = jnp.concatenate([rotated_ref[row] for row in zero_rows], axis=0)
    mixed_ref[...] = dot(merged, band, (0, 0)).reshape(len(zero_rows), channels, edges)
    turned = jnp.concatenate([turned_ref[row] for row in zero_rows], axis=0)
    band_grad_ref[...] = dot(merged, turned, (1, 0)).astype(BF16).reshape(len(zero_rows), channels, edges)

    def back(step, carry):
        at = pl.ds(pl.multiple_of(step * CHUNK, CHUNK), CHUNK)
        gate = gate_ref[at, :]
        values = []
        for row in range(comps):
            if row in zero_rows:
                value = mixed_ref[zero_rows.index(row), at, :]
            else:
                value = rotated_ref[row, at, :].astype(F32)
            values.append((value * gate).astype(BF16).astype(F32))
        for n, total in enumerate(rotate(frames32_ref, range(comps), values, True)):
            gathered_ref[n, at, :] = total
        values = []
        for row in range(comps):
            if row in zero_rows:
                values.append(band_grad_ref[zero_rows.index(row), at, :].astype(F32))
            else:
                values.append(turned_ref[row, at, :].astype(F32))
        for n, total in enumerate(rotate(frames32_ref, range(comps), values, True)):
            back_ref[n, at, :] = total
        return carry

    lax.fori_loop(0, channels // CHUNK, back, 0)
    for j in range(comps):
        summed = dot(incidence, gathered_ref[j].astype(BF16), (1, 1))
        updated_ref[j] = (feats_ref[j].astype(F32) + summed * scale).astype(BF16)
        summed = dot(source, back_ref[j].astype(BF16), (1, 1))
        grad_ref[j] = cot_ref[j].astype(F32) + summed.astype(BF16).astype(F32)


def call(kernel, outs, scratch, flops, *args, space=pltpu.VMEM, out_space=pltpu.VMEM, limit=32 * 1024):
    size = sum(math.prod(a.shape) * a.dtype.itemsize for a in (*args, *outs))
    return pl.pallas_call(
        kernel,
        out_shape=outs,
        in_specs=[pl.BlockSpec(memory_space=space)] * len(args),
        out_specs=[pl.BlockSpec(memory_space=out_space)] * len(outs),
        scratch_shapes=scratch,
        cost_estimate=pl.CostEstimate(flops=flops, bytes_accessed=size, transcendentals=0),
        compiler_params=pltpu.CompilerParams(vmem_limit_bytes=limit * 1024),
    )(*args)


def summed_over_pairs(axis, own, send, copies):
    size = lax.axis_size(axis)
    turns = sorted({1, size - 1})
    for turn in turns:
        other = lax.ppermute(send, axis, [(i, i ^ turn) for i in range(size)])
        last = turn == turns[-1] and copies > 1
        shape = (copies, *own.shape) if last else own.shape
        (own,) = call(pair_kernel, [jax.ShapeDtypeStruct(shape, BF16)], [], 10**6, own, other)
        send = own
    return own


def shards(
    atom_feats,
    cotangent,
    frames,
    radial,
    edge_source,
    edge_target,
    edge_valid,
    atom_types,
    dataset,
    type_table,
    dataset_table,
    router_weight,
    experts,
):
    group = lax.axis_size("shard")
    expert_count, block, width = experts.shape
    atoms, comps, channels = atom_feats.shape
    edges = radial.shape[0]
    degrees = math.isqrt(comps)
    zero_rows = [degree * degree + degree for degree in range(degrees)]
    scale = atoms / edges
    feats = atom_feats.transpose(1, 0, 2)
    cot = cotangent.transpose(1, 0, 2)
    indices = (edge_source[None], edge_target[None], edge_valid[None])
    planes = (comps, channels, edges)
    bands = (degrees, channels, edges)
    common = [
        pltpu.VMEM(frames.shape, F32),
        pltpu.VMEM(planes, F32),
        pltpu.VMEM(planes, F32),
        pltpu.VMEM((channels, edges), F32),
    ]

    def first(*refs):
        first_kernel(zero_rows, scale, *refs)

    columns, cores = lax.axis_size("x"), lax.axis_size("core")
    lanes = 128
    half = expert_count // cores * block
    data = SUB * width // lanes
    lines = data + PARTS
    total_lines = group * columns * lines
    if SUB * columns != block or expert_count > lanes or lines % 2 or cores != 2 or expert_count * data % 16:
        raise ValueError("sizes")
    first_args = (
        atom_types[None],
        dataset[None],
        type_table,
        dataset_table,
        router_weight.T,
        *indices,
        feats,
        cot,
        frames,
        radial,
    )
    (sent,) = call(
        first,
        [jax.ShapeDtypeStruct((total_lines, lanes), BF16)],
        [pltpu.VMEM(a.shape, a.dtype) for a in first_args]
        + common
        + [
            pltpu.VMEM(bands, BF16),
            pltpu.VMEM(bands, BF16),
            pltpu.VMEM((total_lines, lanes), BF16),
            pltpu.SemaphoreType.DMA((len(first_args) + 4,)),
        ],
        10**9,
        *first_args,
        space=pl.ANY,
        out_space=pl.ANY,
        limit=60 * 1024,
    )
    sent = sent.reshape(group * columns, lines // 2, 2, lanes)
    received = lax.all_to_all(sent, ("shard", "x"), 0, 0, tiled=True).reshape(total_lines, lanes)

    def sums_of(*refs):
        sums_kernel(expert_count, group, lines, *refs)

    def shares_of(*refs):
        shares_kernel(block, *refs)

    piece = jax.ShapeDtypeStruct((expert_count // cores * data, lanes), BF16)
    own, send, mine = call(
        sums_of, [piece, piece, jax.ShapeDtypeStruct((PARTS * group, lanes), F32)], [], 10**9, received
    )
    (shares,) = call(
        shares_of,
        [jax.ShapeDtypeStruct((group * block, width), BF16)],
        [pltpu.VMEM((group * block, width), BF16), pltpu.SemaphoreType.DMA((3,))],
        10**9,
        mine,
        experts.reshape(expert_count * block, width),
        out_space=pl.ANY,
    )
    merged = lax.all_to_all(shares.reshape(group, block, width), "shard", 0, 0, tiled=True)
    own = summed_over_pairs("core", own, send, 1)
    own = summed_over_pairs("y", own, own, columns)
    whole = lax.all_to_all(own, "x", 0, 0, tiled=True)

    def layer(*refs):
        layer_kernel(zero_rows, scale, *refs)

    updated, feats_grad = call(
        layer,
        [jax.ShapeDtypeStruct(feats.shape, BF16), jax.ShapeDtypeStruct(feats.shape, F32)],
        common
        + [
            pltpu.VMEM(planes, BF16),
            pltpu.VMEM(planes, BF16),
            pltpu.VMEM(bands, F32),
            pltpu.VMEM(bands, BF16),
        ],
        5 * 10**9,
        feats,
        cot,
        frames,
        radial,
        *indices,
        merged.reshape(group * block, width),
    )
    whole = lax.all_gather(whole, "core", axis=0, tiled=True)

    def join(*refs):
        join_kernel(block, *refs)

    out = jax.ShapeDtypeStruct((expert_count * block, width), F32)
    scratch = [pltpu.VMEM((cores, half, width), F32), pltpu.SemaphoreType.DMA((cores,))]
    (expert_grad,) = call(join, [out], scratch, 10**8, whole, out_space=pl.ANY)
    expert_grad = expert_grad.reshape(expert_count, block, width)
    return (updated.transpose(1, 0, 2), feats_grad.transpose(1, 0, 2), expert_grad)


def solution(mesh):
    shard_size, replica_size = mesh.devices.shape
    if math.prod(REPLICA_SIZES) != replica_size:
        raise ValueError("replica sizes")
    fine = Mesh(mesh.devices.reshape(shard_size, *REPLICA_SIZES), ("shard", "x", "y", "core"))
    both = ("shard", "x", "y", "core")
    in_specs = (
        P(both, None, None),
        P(both, None, None),
        P(None, None, both),
        P(both, None),
        P(both),
        P(both),
        P(both),
        P(both),
        P(both),
        P(),
        P(),
        P(),
        P(None, "shard", None),
    )
    out_specs = (P(both, None, None), P(both, None, None), P(None, "shard", None))
    return jax.shard_map(shards, mesh=fine, in_specs=in_specs, out_specs=out_specs, check_vma=False)
```

```python
import math

import jax
import jax.numpy as jnp
from jax import lax
from jax.experimental import pallas as pl
from jax.experimental.pallas import tpu as pltpu
from jax.sharding import Mesh
from jax.sharding import PartitionSpec as P


BF16 = jnp.bfloat16
F32 = jnp.float32
CHUNK = 16
PARTS = 2
SUB = 4
REPLICA_SIZES = (4, 4, 2)


def iota(shape, dim):
    return lax.broadcasted_iota(jnp.int32, shape, dim)


def dot(a, b, contract):
    return lax.dot_general(a, b, ((contract[:1], contract[1:]), ((), ())), preferred_element_type=F32)


def divided(value, by):
    return jnp.floor((value.astype(F32) + 0.5) * (1.0 / by)).astype(jnp.int32)


def one_hot(index_row, count):
    return iota((count, index_row.shape[1]), 0) == index_row


def split(value):
    parts = []
    for _ in range(PARTS):
        part = value.astype(BF16)
        parts.append(part)
        value = value - part.astype(F32)
    return parts


def mixture_row(types_ref, dataset_ref, type_table_ref, dataset_table_ref, router_ref):
    table = type_table_ref[...]
    atoms = types_ref.shape[1]
    counts = jnp.sum(one_hot(types_ref[...], table.shape[0]).astype(F32), axis=1, keepdims=True)
    embed = jnp.sum(counts * table, axis=0, keepdims=True) / atoms
    data_table = dataset_table_ref[...]
    pick = (iota((data_table.shape[0], 1), 0) == dataset_ref[...]).astype(F32)
    embed = embed + jnp.sum(pick * data_table, axis=0, keepdims=True)
    logits = jnp.sum(router_ref[...] * embed, axis=1, keepdims=True)
    soft = jnp.maximum(logits, 0.0) + jnp.log1p(jnp.exp(-jnp.abs(logits)))
    mixture = soft / jnp.sum(soft, axis=0, keepdims=True)
    shape = (mixture.shape[0], 128)
    return jnp.sum(jnp.where(iota(shape, 0) == iota(shape, 1), mixture, 0.0), axis=0, keepdims=True)


def spread(feats_ref, cot_ref, source_ref, target_ref, valid_ref, gathered_ref, back_ref, scale):
    atoms = feats_ref.shape[1]
    source = one_hot(source_ref[...], atoms).astype(BF16)
    incidence = (one_hot(target_ref[...], atoms) & (valid_ref[...] > 0)).astype(BF16)
    comps = feats_ref.shape[0]
    for j in range(comps):
        gathered_ref[j] = dot(feats_ref[j], source, (0, 0))
        back_ref[j] = dot(cot_ref[j], incidence, (0, 0)) * scale
    return source, incidence


def rotate(frames_ref, rows, values, transposed=False):
    count = len(values)
    out = []
    for i in rows:
        total = None
        for j in range(count):
            row = frames_ref[j, i : i + 1, :] if transposed else frames_ref[i, j : j + 1, :]
            term = row * values[j]
            total = term if total is None else total + term
        out.append(total)
    return out


def first_kernel(zero_rows, scale, *refs):
    count = 12
    sources, (out_ref,), refs = refs[:count], refs[count : count + 1], refs[count + 1 :]
    inputs, refs = refs[:count], refs[count:]
    frames32_ref, gathered_ref, back_ref, gate_ref, band_ref, mixed_ref, held_ref, sems = refs
    copies = [
        pltpu.make_async_copy(source, target, sems.at[n])
        for n, (source, target) in enumerate(zip(sources, inputs))
    ]
    for copy in copies:
        copy.start()
    router_args, edge_args = inputs[:5], inputs[5:]
    pieces = len(zero_rows)
    lines = SUB * pieces + PARTS
    batch = 8
    rows = batch * lines
    line = iota((rows, 1), 0)
    message = divided(line, lines)
    line = line - message * lines
    data = SUB * pieces
    wanted = jnp.where(
        line < data,
        batch * SUB * (line // SUB) + SUB * message + line % SUB,
        batch * data + line - data,
    )
    place = (iota((rows, batch * data + 16), 1) == wanted).astype(BF16)
    for copy in copies:
        copy.wait()
    row = mixture_row(*router_args)
    source_ref, target_ref, valid_ref, feats_ref, cot_ref, frames_ref, radial_ref = edge_args
    comps, _, channels = feats_ref.shape
    frames32_ref[...] = frames_ref[...].astype(F32)
    gate_ref[...] = radial_ref[...].astype(F32).T
    spread(feats_ref, cot_ref, source_ref, target_ref, valid_ref, gathered_ref, back_ref, scale)

    def chunk(step, carry):
        at = pl.ds(pl.multiple_of(step * CHUNK, CHUNK), CHUNK)
        values = [gathered_ref[j, at, :] for j in range(comps)]
        for n, total in enumerate(rotate(frames32_ref, zero_rows, values)):
            band_ref[n, at, :] = total.astype(BF16)
        values = [back_ref[j, at, :] for j in range(comps)]
        gate = gate_ref[at, :]
        for n, total in enumerate(rotate(frames32_ref, zero_rows, values)):
            mixed_ref[n, at, :] = (total.astype(BF16).astype(F32) * gate).astype(BF16)
        return carry

    lax.fori_loop(0, channels // CHUNK, chunk, 0, unroll=True)
    edges = band_ref.shape[2]
    band = band_ref[...].reshape(-1, edges)
    grads = [dot(band, mixed_ref[n], (1, 1)).astype(BF16) for n in range(pieces)]
    tail = jnp.concatenate([part.astype(F32) for part in split(row)] + [jnp.zeros((16 - PARTS, channels), F32)], axis=0)
    tail = tail.astype(BF16)
    steps = band.shape[0] // (batch * SUB)
    chunk_steps = steps // (sems.shape[0] - count)
    for step in range(steps):
        at = slice(step * batch * SUB, (step + 1) * batch * SUB)
        stack = jnp.concatenate([grad[at] for grad in grads] + [tail], axis=0)
        held_ref[step * rows : (step + 1) * rows] = dot(place, stack, (1, 0)).astype(BF16)
        if (step + 1) % chunk_steps == 0:
            done = pl.ds((step + 1 - chunk_steps) * rows, chunk_steps * rows)
            copies.append(pltpu.make_async_copy(held_ref.at[done], out_ref.at[done], sems.at[len(copies)]))
            copies[-1].start()
    for copy in copies[count:]:
        copy.wait()


def sums_kernel(expert_count, group, lines, recv_ref, own_ref, send_ref, mine_ref):
    total_lines, lanes = recv_ref.shape
    systems = total_lines // lines
    columns = systems // group
    data = lines - PARTS
    rows = expert_count * data
    values = recv_ref[...]
    shape = (systems, total_lines)
    picks = [iota(shape, 1) == iota(shape, 0) * lines + data]
    shape = (group, total_lines)
    for p in range(PARTS):
        start = lax.axis_index("x") * lines + data + p
        picks.append(iota(shape, 1) == iota(shape, 0) * (columns * lines) + start)
    picked = dot(jnp.concatenate([pick.astype(F32) for pick in picks], axis=0).astype(BF16), values, (1, 0))
    mine_ref[...] = picked[systems:]
    column = iota((1, total_lines), 1)
    system = divided(column, lines)
    row = iota((rows, 1), 0)
    expert = divided(row, data)
    collect_experts = (iota((rows, lanes), 1) == expert).astype(BF16)
    collect_systems = (iota((systems, total_lines), 0) == system).astype(BF16)
    narrow = dot(collect_experts, picked[:systems].astype(BF16), (1, 1)).astype(BF16)
    same = row - expert * data == column - system * lines
    weights = jnp.where(same, dot(narrow, collect_systems, (1, 0)), 0.0).astype(BF16)
    total = dot(weights, values, (1, 0))
    half = rows // 2
    first = lax.axis_index("core") == 0
    own_ref[...] = jnp.where(first, total[:half], total[half:]).astype(BF16)
    send_ref[...] = jnp.where(first, total[half:], total[:half]).astype(BF16)


def shares_kernel(block, mine_ref, experts_ref, shares_ref, held_ref, sems):
    group = mine_ref.shape[0] // PARTS
    lanes = mine_ref.shape[1]
    total_rows = experts_ref.shape[0]
    chunks = sems.shape[0]
    rows = group * block // chunks
    shape = (lanes, total_rows)
    spread_experts = (iota(shape, 1) // block == iota(shape, 0)).astype(BF16)
    same = iota((rows, 1), 0) % block == iota((1, total_rows), 1) % block
    experts = experts_ref[...]
    parts = [mine_ref[p * group : (p + 1) * group, :].astype(BF16) for p in range(PARTS)]
    wide = [dot(part, spread_experts, (1, 0)).astype(BF16) for part in parts]
    copies = []
    for n in range(chunks):
        at = pl.ds(n * rows, rows)
        shape = (rows, group)
        spread_systems = ((iota(shape, 0) + n * rows) // block == iota(shape, 1)).astype(BF16)
        weights = [jnp.where(same, dot(spread_systems, part, (1, 0)), 0.0).astype(BF16) for part in wide]
        terms = dot(jnp.concatenate(weights, axis=0), experts, (1, 0))
        shares = sum(terms[p * rows : (p + 1) * rows] for p in range(PARTS))
        held_ref[at, :] = shares.astype(BF16)
        copies.append(pltpu.make_async_copy(held_ref.at[at, :], shares_ref.at[at, :], sems.at[n]))
        copies[-1].start()
    for copy in copies:
        copy.wait()


def join_kernel(block, parts_ref, out_ref, held_ref, sems):
    cores, half, width = held_ref.shape
    columns = block // SUB
    lanes = parts_ref.shape[2]
    pieces = width // lanes
    data = SUB * pieces
    low = iota((2 * SUB, lanes), 0) < SUB
    copies = []

    def turned(value, line, place):
        at = line // (2 * SUB) * 2 * SUB
        value = value[at : at + 2 * SUB]
        return value if line - at == place else pltpu.roll(value, SUB, 0)

    for core in range(cores):
        values = [parts_ref[core * columns + column].astype(F32) for column in range(columns)]
        for expert in range(half // block):
            for piece in range(pieces):
                line = expert * data + piece * SUB
                for column in range(0, columns, 2):
                    upper = turned(values[column], line, 0)
                    lower = turned(values[column + 1], line, SUB)
                    at = expert * block + column * SUB
                    held_ref[core, at : at + 2 * SUB, piece * lanes : (piece + 1) * lanes] = jnp.where(low, upper, lower)
        copies.append(
            pltpu.make_async_copy(held_ref.at[core], out_ref.at[pl.ds(core * half, half), :], sems.at[core])
        )
        copies[-1].start()
    for copy in copies:
        copy.wait()


def pair_kernel(own_ref, other_ref, out_ref):
    total = (own_ref[...].astype(F32) + other_ref[...].astype(F32)).astype(BF16)
    out_ref[...] = jnp.broadcast_to(total, out_ref.shape)


def layer_kernel(
    zero_rows,
    scale,
    feats_ref,
    cot_ref,
    frames_ref,
    radial_ref,
    source_ref,
    target_ref,
    valid_ref,
    merged_ref,
    updated_ref,
    grad_ref,
    frames32_ref,
    gathered_ref,
    back_ref,
    gate_ref,
    rotated_ref,
    turned_ref,
    mixed_ref,
    band_grad_ref,
):
    comps, _, channels = feats_ref.shape
    edges = radial_ref.shape[0]
    frames32_ref[...] = frames_ref[...].astype(F32)
    gate_ref[...] = radial_ref[...].astype(F32).T
    source, incidence = spread(
        feats_ref, cot_ref, source_ref, target_ref, valid_ref, gathered_ref, back_ref, scale
    )

    def forth(step, carry):
        at = pl.ds(pl.multiple_of(step * CHUNK, CHUNK), CHUNK)
        values = [gathered_ref[j, at, :] for j in range(comps)]
        for n, total in enumerate(rotate(frames32_ref, range(comps), values)):
            rotated_ref[n, at, :] = total.astype(BF16)
        values = [back_ref[j, at, :] for j in range(comps)]
        gate = gate_ref[at, :]
        for n, total in enumerate(rotate(frames32_ref, range(comps), values)):
            turned_ref[n, at, :] = (total.astype(BF16).astype(F32) * gate).astype(BF16)
        return carry

    lax.fori_loop(0, channels // CHUNK, forth, 0)
    merged = merged_ref[...]
    band = jnp.concatenate([rotated_ref[row] for row in zero_rows], axis=0)
    mixed_ref[...] = dot(merged, band, (0, 0)).reshape(len(zero_rows), channels, edges)
    turned = jnp.concatenate([turned_ref[row] for row in zero_rows], axis=0)
    band_grad_ref[...] = dot(merged, turned, (1, 0)).astype(BF16).reshape(len(zero_rows), channels, edges)

    def back(step, carry):
        at = pl.ds(pl.multiple_of(step * CHUNK, CHUNK), CHUNK)
        gate = gate_ref[at, :]
        values = []
        for row in range(comps):
            if row in zero_rows:
                value = mixed_ref[zero_rows.index(row), at, :]
            else:
                value = rotated_ref[row, at, :].astype(F32)
            values.append((value * gate).astype(BF16).astype(F32))
        for n, total in enumerate(rotate(frames32_ref, range(comps), values, True)):
            gathered_ref[n, at, :] = total
        values = []
        for row in range(comps):
            if row in zero_rows:
                values.append(band_grad_ref[zero_rows.index(row), at, :].astype(F32))
            else:
                values.append(turned_ref[row, at, :].astype(F32))
        for n, total in enumerate(rotate(frames32_ref, range(comps), values, True)):
            back_ref[n, at, :] = total
        return carry

    lax.fori_loop(0, channels // CHUNK, back, 0)
    for j in range(comps):
        summed = dot(incidence, gathered_ref[j].astype(BF16), (1, 1))
        updated_ref[j] = (feats_ref[j].astype(F32) + summed * scale).astype(BF16)
        summed = dot(source, back_ref[j].astype(BF16), (1, 1))
        grad_ref[j] = cot_ref[j].astype(F32) + summed.astype(BF16).astype(F32)


def call(kernel, outs, scratch, flops, *args, space=pltpu.VMEM, out_space=pltpu.VMEM, limit=32 * 1024):
    size = sum(math.prod(a.shape) * a.dtype.itemsize for a in (*args, *outs))
    return pl.pallas_call(
        kernel,
        out_shape=outs,
        in_specs=[pl.BlockSpec(memory_space=space)] * len(args),
        out_specs=[pl.BlockSpec(memory_space=out_space)] * len(outs),
        scratch_shapes=scratch,
        cost_estimate=pl.CostEstimate(flops=flops, bytes_accessed=size, transcendentals=0),
        compiler_params=pltpu.CompilerParams(vmem_limit_bytes=limit * 1024),
    )(*args)


def summed_over_pairs(axis, own, send, copies):
    size = lax.axis_size(axis)
    turns = sorted({1, size - 1})
    for turn in turns:
        other = lax.ppermute(send, axis, [(i, i ^ turn) for i in range(size)])
        last = turn == turns[-1] and copies > 1
        shape = (copies, *own.shape) if last else own.shape
        (own,) = call(pair_kernel, [jax.ShapeDtypeStruct(shape, BF16)], [], 10**6, own, other)
        send = own
    return own


def shards(
    atom_feats,
    cotangent,
    frames,
    radial,
    edge_source,
    edge_target,
    edge_valid,
    atom_types,
    dataset,
    type_table,
    dataset_table,
    router_weight,
    experts,
):
    group = lax.axis_size("shard")
    expert_count, block, width = experts.shape
    atoms, comps, channels = atom_feats.shape
    edges = radial.shape[0]
    degrees = math.isqrt(comps)
    zero_rows = [degree * degree + degree for degree in range(degrees)]
    scale = atoms / edges
    feats = atom_feats.transpose(1, 0, 2)
    cot = cotangent.transpose(1, 0, 2)
    indices = (edge_source[None], edge_target[None], edge_valid[None])
    planes = (comps, channels, edges)
    bands = (degrees, channels, edges)
    common = [
        pltpu.VMEM(frames.shape, F32),
        pltpu.VMEM(planes, F32),
        pltpu.VMEM(planes, F32),
        pltpu.VMEM((channels, edges), F32),
    ]

    def first(*refs):
        first_kernel(zero_rows, scale, *refs)

    columns, cores = lax.axis_size("x"), lax.axis_size("core")
    lanes = 128
    half = expert_count // cores * block
    data = SUB * width // lanes
    lines = data + PARTS
    total_lines = group * columns * lines
    if SUB * columns != block or expert_count > lanes or lines % 2 or cores != 2 or expert_count * data % 16:
        raise ValueError("sizes")
    first_args = (
        atom_types[None],
        dataset[None],
        type_table,
        dataset_table,
        router_weight.T,
        *indices,
        feats,
        cot,
        frames,
        radial,
    )
    (sent,) = call(
        first,
        [jax.ShapeDtypeStruct((total_lines, lanes), BF16)],
        [pltpu.VMEM(a.shape, a.dtype) for a in first_args]
        + common
        + [
            pltpu.VMEM(bands, BF16),
            pltpu.VMEM(bands, BF16),
            pltpu.VMEM((total_lines, lanes), BF16),
            pltpu.SemaphoreType.DMA((len(first_args) + 4,)),
        ],
        10**9,
        *first_args,
        space=pl.ANY,
        out_space=pl.ANY,
        limit=60 * 1024,
    )
    sent = sent.reshape(group * columns, lines // 2, 2, lanes)
    received = lax.all_to_all(sent, ("shard", "x"), 0, 0, tiled=True).reshape(total_lines, lanes)

    def sums_of(*refs):
        sums_kernel(expert_count, group, lines, *refs)

    def shares_of(*refs):
        shares_kernel(block, *refs)

    piece = jax.ShapeDtypeStruct((expert_count // cores * data, lanes), BF16)
    own, send, mine = call(
        sums_of, [piece, piece, jax.ShapeDtypeStruct((PARTS * group, lanes), F32)], [], 10**9, received
    )
    (shares,) = call(
        shares_of,
        [jax.ShapeDtypeStruct((group * block, width), BF16)],
        [pltpu.VMEM((group * block, width), BF16), pltpu.SemaphoreType.DMA((2,))],
        10**9,
        mine,
        experts.reshape(expert_count * block, width),
        out_space=pl.ANY,
    )
    merged = lax.all_to_all(shares.reshape(group, block, width), "shard", 0, 0, tiled=True)
    own = summed_over_pairs("core", own, send, 1)
    own = summed_over_pairs("y", own, own, columns)
    whole = lax.all_to_all(own, "x", 0, 0, tiled=True)

    def layer(*refs):
        layer_kernel(zero_rows, scale, *refs)

    updated, feats_grad = call(
        layer,
        [jax.ShapeDtypeStruct(feats.shape, BF16), jax.ShapeDtypeStruct(feats.shape, F32)],
        common
        + [
            pltpu.VMEM(planes, BF16),
            pltpu.VMEM(planes, BF16),
            pltpu.VMEM(bands, F32),
            pltpu.VMEM(bands, BF16),
        ],
        5 * 10**9,
        feats,
        cot,
        frames,
        radial,
        *indices,
        merged.reshape(group * block, width),
    )
    whole = lax.all_gather(whole, "core", axis=0, tiled=True)

    def join(*refs):
        join_kernel(block, *refs)

    out = jax.ShapeDtypeStruct((expert_count * block, width), F32)
    scratch = [pltpu.VMEM((cores, half, width), F32), pltpu.SemaphoreType.DMA((cores,))]
    (expert_grad,) = call(join, [out], scratch, 10**8, whole, out_space=pl.ANY)
    expert_grad = expert_grad.reshape(expert_count, block, width)
    return (updated.transpose(1, 0, 2), feats_grad.transpose(1, 0, 2), expert_grad)


def solution(mesh):
    shard_size, replica_size = mesh.devices.shape
    if math.prod(REPLICA_SIZES) != replica_size:
        raise ValueError("replica sizes")
    fine = Mesh(mesh.devices.reshape(shard_size, *REPLICA_SIZES), ("shard", "x", "y", "core"))
    both = ("shard", "x", "y", "core")
    in_specs = (
        P(both, None, None),
        P(both, None, None),
        P(None, None, both),
        P(both, None),
        P(both),
        P(both),
        P(both),
        P(both),
        P(both),
        P(),
        P(),
        P(),
        P(None, "shard", None),
    )
    out_specs = (P(both, None, None), P(both, None, None), P(None, "shard", None))
    return jax.shard_map(shards, mesh=fine, in_specs=in_specs, out_specs=out_specs, check_vma=False)
```
